512 devices in a mesh: ctx: 64 (over z, y_lo, core), tp: 8 (over x, y_hi).
Axes of the slice: x: 4, y: 4 (y_hi: 2, y_lo: 2; y = y_hi * 2 + y_lo), z: 16, core: 2. Of those that a mesh axis runs over, the one named last changes fastest.
Arguments:
- query_se: bfloat16 [14336, 8192], P('ctx', 'tp'), may hold values from -6 to 6
- key_se: bfloat16 [14336, 8192], P('ctx', 'tp'), may hold values from -6 to 6
- value_se: bfloat16 [14336, 8192], P('ctx', 'tp'), may hold values from -6 to 6
- query_mr: bfloat16 [14336, 8192], P('ctx', 'tp'), may hold values from -6 to 6
- key_mr: bfloat16 [14336, 8192], P('ctx', 'tp'), may hold values from -6 to 6
- upstream: bfloat16 [14336, 8192], P('ctx', 'tp'), may hold values from -6 to 6
- filter_se: float32 [7, 8192], P(None, 'tp'), may hold values from -2 to 2
- filter_mr: float32 [128, 8192], P(None, 'tp'), may hold values from -0.5 to 0.5
- skip_mr: float32 [8192], P('tp'), may hold values from -1 to 1
- norm_gain: float32 [8192], P('tp'), may hold values from 0.1 to 1.9
Outputs:
- grad_query_se: bfloat16 [14336, 8192], P('ctx', 'tp')
- grad_key_se: bfloat16 [14336, 8192], P('ctx', 'tp')
- grad_value_se: bfloat16 [14336, 8192], P('ctx', 'tp')
- grad_query_mr: bfloat16 [14336, 8192], P('ctx', 'tp')
- grad_key_mr: bfloat16 [14336, 8192], P('ctx', 'tp')
- grad_filter_se: float32 [7, 8192], P(None, ('tp', 'ctx'))
- grad_filter_mr: float32 [128, 8192], P(None, ('tp', 'ctx'))
- grad_skip: float32 [8192], P(('tp', 'ctx'))
- grad_gain: float32 [8192], P(('tp', 'ctx'))
The draws below stay inside these ranges and needn't reach their ends.
All inputs are finite; a program needn't handle non-finite values.
Results may differ from the reference program's by a relative error of at most 0.0062.
Values may be sent and summed in bfloat16 or wider, within the bound.
No kernel may reach another device: no remote copies, remote signals or barrier semaphores. Data moves between devices by JAX's collectives and lax.ppermute only.
A program may use at most 64 MiB of HBM per device.

```python
import math
import jax
import jax.numpy as jnp
from jax import lax

D = 8192
SE_TAPS = 7
MR_TAPS = 128
TOKENS = 14336


def block_scale(rng, dims, split, least, high):
    loudness, own = 1.0, jax.random.fold_in(rng, 6)
    for dim, blocks in split:
        heights = jnp.exp(jax.random.uniform(jax.random.fold_in(own, dim), (blocks,), jnp.float32, least / len(split), high / len(split)))
        loudness = loudness * jnp.repeat(heights, dims[dim] // blocks).reshape([-1 if axis == dim else 1 for axis in range(len(dims))])
    return loudness


def bell_draw(key, extent, scale, limit, pieces=(), kind=jnp.bfloat16):
    loudness = block_scale(key, extent, pieces, -0.22, 0.18) if pieces else 1.0
    drawn = jax.random.normal(key, extent, jnp.float32) * scale * loudness
    return jnp.minimum(jnp.maximum(drawn, -limit), limit).astype(kind)


def setup_inputs(seed: int = 0) -> dict:
    streams_of = jax.random.split(jax.random.key(seed), 11)
    query_se = bell_draw(streams_of[0], (TOKENS, D), 1.0, 6.0, ((0, 64), (1, 8)))
    key_se = bell_draw(streams_of[1], (TOKENS, D), 1.0, 6.0, ((0, 64), (1, 8)))
    value_se = bell_draw(streams_of[2], (TOKENS, D), 1.0, 6.0, ((0, 64), (1, 8)))
    query_mr = bell_draw(streams_of[3], (TOKENS, D), 1.0, 6.0, ((0, 64), (1, 8)))
    key_mr = bell_draw(streams_of[4], (TOKENS, D), 1.0, 6.0, ((0, 64), (1, 8)))
    upstream = bell_draw(streams_of[5], (TOKENS, D), 1.0, 6.0, ((0, 64), (1, 8)))
    filter_se = bell_draw(streams_of[6], (SE_TAPS, D), SE_TAPS ** -0.5, 2.0, ((1, 8),), jnp.float32)
    filter_mr = bell_draw(streams_of[7], (MR_TAPS, D), MR_TAPS ** -0.5, 0.5, ((1, 8),), jnp.float32)
    skip_mr = jnp.clip(jax.random.uniform(streams_of[8], (D,), jnp.float32, -1.0, 1.0) * block_scale(streams_of[8], (D,), ((0, 8),), -0.4, 0.0), -1.0, 1.0)
    norm_gain = jnp.clip(1.0 + 0.18 * jax.random.normal(streams_of[9], (D,), jnp.float32), 0.1, 1.9)
    return {"query_se": query_se, "key_se": key_se, "value_se": value_se, "query_mr": query_mr, "key_mr": key_mr, "upstream": upstream, "filter_se": filter_se, "filter_mr": filter_mr, "skip_mr": skip_mr, "norm_gain": norm_gain}


EPSILON = 0.1

def rounded(value):
    half = lax.optimization_barrier(value.astype(jnp.bfloat16))
    return half.astype(jnp.float32)

def to_blocks(array, width):
    rows, chans = array.shape
    return array.reshape(rows, chans // width, width).transpose(1, 0, 2)

def from_blocks(array):
    count, rows, width = array.shape
    return array.transpose(1, 0, 2).reshape(rows, count * width)

def shift_down(field, steps):
    zeros = jnp.zeros((steps, field.shape[1]), field.dtype)
    return jnp.concatenate([zeros, field[:field.shape[0] - steps]], 0)

def shift_up(field, steps):
    zeros = jnp.zeros((steps, field.shape[1]), field.dtype)
    return jnp.concatenate([field[steps:], zeros], 0)

def short_conv(field, taps):
    result = taps[0] * field
    for step in range(1, taps.shape[0]):
        result = result + taps[step] * shift_down(field, step)
    return result

def short_adjoint(field, taps):
    result = taps[0] * field
    for step in range(1, taps.shape[0]):
        result = result + taps[step] * shift_up(field, step)
    return result

def short_corr(grads, field, count):
    return jnp.stack([lax.optimization_barrier(jnp.sum(grads * shift_down(field, step), axis=0)) for step in range(count)], 0)

def long_conv(field, taps, length):
    spectrum = jnp.fft.rfft(field, n=length, axis=0) * jnp.fft.rfft(taps, n=length, axis=0)
    return jnp.fft.irfft(spectrum, n=length, axis=0)[:field.shape[0]]

def long_adjoint(field, taps, length):
    spectrum = jnp.fft.rfft(field, n=length, axis=0) * jnp.conj(jnp.fft.rfft(taps, n=length, axis=0))
    return jnp.fft.irfft(spectrum, n=length, axis=0)[:field.shape[0]]

def long_corr(grads, field, length, count):
    spectrum = jnp.fft.rfft(grads, n=length, axis=0) * jnp.conj(jnp.fft.rfft(field, n=length, axis=0))
    return jnp.fft.irfft(spectrum, n=length, axis=0)[:count]

def reference(query_se, key_se, value_se, query_mr, key_mr, upstream, filter_se, filter_mr, skip_mr, norm_gain):
    width = math.gcd(D, 1024)
    count = D // width
    length = TOKENS + MR_TAPS
    b_qse = to_blocks(query_se, width)
    b_kse = to_blocks(key_se, width)
    b_vse = to_blocks(value_se, width)
    b_qmr = to_blocks(query_mr, width)
    b_kmr = to_blocks(key_mr, width)
    b_up = to_blocks(upstream, width)
    b_fse = to_blocks(filter_se, width)
    b_fmr = to_blocks(filter_mr, width)
    b_skip = skip_mr.reshape(count, width)
    b_gain = norm_gain.reshape(count, width)

    def short_layer(query, keys, values, taps):
        product = rounded(keys.astype(jnp.float32) * values.astype(jnp.float32))
        conv = short_conv(product, taps)
        return (product, conv, query.astype(jnp.float32) * conv)

    def first(items):
        query, keys, values, taps = items
        product, conv, mixed = short_layer(query, keys, values, taps)
        return lax.optimization_barrier(jnp.sum(mixed * mixed, axis=1))
    squares = lax.optimization_barrier(jnp.sum(lax.map(first, (b_qse, b_kse, b_vse, b_fse)), axis=0))
    scale_rows = lax.rsqrt(squares / D + EPSILON)

    def second(items):
        query, keys, values, taps, gate_q, gate_k, cotan, long_taps, skip, gain = items
        product, conv, mixed = short_layer(query, keys, values, taps)
        normed = mixed * scale_rows[:, None] * gain
        product_mr = rounded(gate_k.astype(jnp.float32) * normed)
        conv_mr = long_conv(product_mr, long_taps, length) + skip * product_mr
        cot = cotan.astype(jnp.float32)
        grad_query_mr = (cot * conv_mr).astype(jnp.bfloat16)
        grad_conv_mr = rounded(cot * gate_q.astype(jnp.float32))
        grad_product_mr = long_adjoint(grad_conv_mr, long_taps, length) + skip * grad_conv_mr
        grad_key_mr = (grad_product_mr * normed).astype(jnp.bfloat16)
        grad_normed = grad_product_mr * gate_k.astype(jnp.float32)
        weighted = lax.optimization_barrier(jnp.sum(grad_normed * gain * mixed, axis=1))
        grad_filter_mr = long_corr(grad_conv_mr, product_mr, length, MR_TAPS)
        grad_skip = lax.optimization_barrier(jnp.sum(grad_conv_mr * product_mr, axis=0))
        grad_gain = lax.optimization_barrier(jnp.sum(grad_normed * mixed * scale_rows[:, None], axis=0))
        return (grad_query_mr, grad_key_mr, grad_normed, weighted, grad_filter_mr, grad_skip, grad_gain)
    out_b = lax.map(second, (b_qse, b_kse, b_vse, b_fse, b_qmr, b_kmr, b_up, b_fmr, b_skip, b_gain))
    grad_query_mr, grad_key_mr, grad_normed, weighted, grad_filter_mr, grad_skip, grad_gain = out_b
    weighted = lax.optimization_barrier(jnp.sum(weighted, axis=0))

    def third(items):
        query, keys, values, taps, gain, back = items
        product, conv, mixed = short_layer(query, keys, values, taps)
        grad_mixed = gain * scale_rows[:, None] * back - mixed * (scale_rows ** 3 * weighted / D)[:, None]
        grad_query_se = (grad_mixed * conv).astype(jnp.bfloat16)
        grad_conv_se = rounded(grad_mixed * query.astype(jnp.float32))
        grad_product_se = short_adjoint(grad_conv_se, taps)
        grad_key_se = (grad_product_se * values.astype(jnp.float32)).astype(jnp.bfloat16)
        grad_value_se = (grad_product_se * keys.astype(jnp.float32)).astype(jnp.bfloat16)
        grad_filter_se = short_corr(grad_conv_se, product, SE_TAPS)
        return (grad_query_se, grad_key_se, grad_value_se, grad_filter_se)
    grad_query_se, grad_key_se, grad_value_se, grad_filter_se = lax.map(third, (b_qse, b_kse, b_vse, b_fse, b_gain, grad_normed))
    factor = 1.0 / math.sqrt(TOKENS)
    return (from_blocks(grad_query_se), from_blocks(grad_key_se), from_blocks(grad_value_se), from_blocks(grad_query_mr), from_blocks(grad_key_mr), from_blocks(grad_filter_se) * factor, from_blocks(grad_filter_mr) * factor, grad_skip.reshape(D) * factor, grad_gain.reshape(D) * factor)
```

```python
import math

import jax
import jax.numpy as jnp
import numpy as np
from jax import lax
from jax.experimental import pallas as pl
from jax.experimental.pallas import tpu as pltpu
from jax.sharding import PartitionSpec as P

D = 8192
EPSILON = 0.1
BF = jnp.bfloat16
F32 = jnp.float32

LEN = 384
HALF = LEN // 2
ROWS = 224
EXT = ROWS + 8
HALO = 128
HEAD = 136
CB = 256
FWD = HALO + 8 + 8
BWD = HEAD + 24
CHUNK = 32


def basis(first, last):
    theta = np.pi * (2 * np.arange(HALF)[:, None] + 1) / LEN * np.arange(first, last)[None, :]
    return np.concatenate([np.cos(theta), -np.sin(theta)], 0)


def halves(matrix):
    high = matrix.astype(BF)
    low = (matrix - high.astype(np.float64)).astype(BF)
    return high, low


def dot(a, b):
    return jnp.dot(a, b, preferred_element_type=F32)


def split(x):
    high = x.astype(BF)
    return high, (x - high.astype(F32)).astype(BF)


def forward(fh, fl, data):
    return dot(fh, data) + dot(fl, data)


def inverse(th, tl, spectrum):
    high, low = split(spectrum)
    return dot(th, high) + dot(tl, high) + dot(th, low)


def wide(column):
    return jnp.concatenate([column] * (CB // 128), axis=1)


def folded(x):
    total = x[:, :128]
    for at in range(128, x.shape[1], 128):
        total = total + x[:, at : at + 128]
    return total


def sums_in_lanes(acc):
    ones = jnp.ones((8, 128), F32)
    return lax.dot_general(
        ones, acc, (((1,), (1,)), ((), ())), precision=lax.Precision.HIGHEST, preferred_element_type=F32
    )


def short_conv(ref, taps, row, count):
    total = None
    for step in range(7):
        term = taps[step : step + 1, :] * ref[pl.ds(row - step, count), :]
        total = term if total is None else total + term
    return total


def short_adjoint(ref, taps, row, count):
    total = None
    for step in range(7):
        term = taps[step : step + 1, :] * ref[pl.ds(row + step, count), :]
        total = term if total is None else total + term
    return total


def rounded(x):
    return x.astype(BF).astype(F32)


def send_kernel(kse, vse, qse, kmr, up, qmr, fse, gain, fwd, bwd, prod, acc):
    i = pl.program_id(0)
    first = ROWS - HALO - 16
    tail = rounded(kse[first:].astype(F32) * vse[first:].astype(F32))
    prod[...] = tail
    taps = fse[...]

    @pl.when(i == 0)
    def _():
        acc[...] = jnp.zeros_like(acc)

    for r in range(0, HALO, CHUNK):
        conv = short_conv(prod, taps, 16 + r, CHUNK)
        at = ROWS - HALO + r
        mixed = qse[at : at + CHUNK].astype(F32) * conv
        fwd[r : r + CHUNK] = (kmr[at : at + CHUNK].astype(F32) * mixed * gain[...]).astype(BF)
        acc[r : r + CHUNK] += folded(mixed * mixed)
    fwd[HALO : HALO + 8] = tail[HALO + 8 :].astype(BF)
    fwd[HALO + 8 :] = jnp.zeros((8, CB), BF)
    bwd[:HEAD] = (up[:HEAD].astype(F32) * qmr[:HEAD].astype(F32)).astype(BF)
    bwd[HEAD : HEAD + 8] = qse[:8]
    bwd[HEAD + 8 : HEAD + 16] = kmr[:8]
    bwd[HEAD + 16 :] = (kse[:8].astype(F32) * vse[:8].astype(F32)).astype(BF)

    @pl.when(i == pl.num_programs(0) - 1)
    def _():
        total = sums_in_lanes(acc[...])
        high = total.astype(BF).astype(F32)
        rows = lax.broadcasted_iota(jnp.int32, (8, 128), 0)
        fwd[HALO + 8 :, :128] = jnp.where(rows == 0, high, jnp.where(rows == 1, total - high, 0.0)).astype(BF)


def local_kernel(up, qmr, fmr, fxh, fxl, gloc, hspec):
    g = (up[...].astype(F32) * qmr[...].astype(F32)).astype(BF)
    gloc[...] = forward(fxh[:, HALO:], fxl[:, HALO:], g)
    high, low = split(fmr[...])
    fh = fxh[:, HALO : HALO + 128]
    hspec[...] = dot(fh, high) + dot(fxl[:, HALO : HALO + 128], high) + dot(fh, low)


def norm_kernel(
    fwd, bwd, kse, vse, qse, kmr, up, qmr, fse, gain, skip, gloc, hspec, fhh, fhl, th, tl,
    mixed_o, conv_o, gp_o, stats, prod, tail, acc_sq, acc_w
):
    i = pl.program_id(0)
    last = pl.num_programs(0) - 1

    @pl.when(i == 0)
    def _():
        acc_sq[...] = jnp.zeros_like(acc_sq)
        acc_w[...] = jnp.zeros_like(acc_w)

    prod[:8] = fwd[HALO : HALO + 8].astype(F32)
    prod[8 : 8 + ROWS] = rounded(kse[...].astype(F32) * vse[...].astype(F32))
    prod[8 + ROWS :] = bwd[HEAD + 16 :].astype(F32)
    spec = gloc[...] + forward(fhh[...], fhl[...], bwd[:HEAD])
    h = hspec[...]
    gr, gi, hr, hi = spec[:HALF], spec[HALF:], h[:HALF], h[HALF:]
    back = jnp.concatenate([gr * hr + gi * hi, gi * hr - gr * hi], 0)
    gp_o[...] = inverse(th[...], tl[...], back)
    taps = fse[...]

    def rows(at, count, query, key, g):
        conv = short_conv(prod, taps, 8 + at, count)
        conv_o[at : at + count] = conv
        mixed = query.astype(F32) * conv
        mixed_o[at : at + count] = mixed
        gp = gp_o[at : at + count] + skip[...] * g.astype(F32)
        gp_o[at : at + count] = gp
        acc_sq[at : at + count] += folded(mixed * mixed)
        acc_w[at : at + count] += folded(gp * key.astype(F32) * gain[...] * mixed)

    for at in range(0, ROWS, CHUNK):
        s = slice(at, at + CHUNK)
        rows(at, CHUNK, qse[s], kmr[s], rounded(up[s].astype(F32) * qmr[s].astype(F32)))
    rows(ROWS, 8, bwd[HEAD : HEAD + 8], bwd[HEAD + 8 : HEAD + 16], bwd[:8])

    @pl.when(i == last)
    def _():
        sq = sums_in_lanes(acc_sq[...])
        w = sums_in_lanes(acc_w[...])
        sent = fwd[HALO + 8 :, :128].astype(F32)
        tail[...] = jnp.concatenate(
            [sq[:1, :128], sq[:1, 128:], w[:1, :128], w[:1, 128:], sent[:1] + sent[1:2], jnp.zeros((3, 128), F32)], 0
        )
        for dev in range(8):
            stats[dev] = tail[...]


def column(total, row):
    pick = (lax.broadcasted_iota(jnp.int32, (8, 128), 0) == row).astype(F32)
    return lax.dot_general(
        total, pick, (((0,), (0,)), ((), ())), precision=lax.Precision.HIGHEST, preferred_element_type=F32
    )


def filter_kernel(
    stats, fwd, mixed, gp, kmr, qse, up, qmr, kse, vse, bwd, gain, gloc, fxh, fxl, th, tl,
    payload, xspec, gc_o, scale_o, coef_o, prod, halo_s, small, xin
):
    i = pl.program_id(0)
    last = pl.num_programs(0) - 1

    @pl.when(i == 0)
    def _():
        total = stats[0]
        for dev in range(1, 8):
            total = total + stats[dev]
        s0 = lax.rsqrt(column(total, 0) / D + EPSILON)
        s1 = lax.rsqrt(column(total, 1) / D + EPSILON)
        scale_o[:128] = s0
        scale_o[128:] = s1[: EXT - 128]
        coef_o[:128] = s0 * s0 * s0 * (column(total, 2) / D)
        coef_o[128:] = (s1 * s1 * s1 * (column(total, 3) / D))[: EXT - 128]
        halo_s[...] = lax.rsqrt(column(total, 4) / D + EPSILON)

    for at in range(0, HALO, CHUNK):
        s = slice(at, at + CHUNK)
        xin[s] = (fwd[s].astype(F32) * wide(halo_s[s])).astype(BF)
    prod[:8] = fwd[HALO : HALO + 8].astype(F32)
    prod[8:] = rounded(kse[...].astype(F32) * vse[...].astype(F32))

    gains = gain[...]
    sums = [jnp.zeros((8, CB), F32) for _ in range(9)]

    def eights(x):
        total = x[:8]
        for r in range(8, x.shape[0], 8):
            total = total + x[r : r + 8]
        return total

    def rows(at, count, query, key):
        scale = wide(scale_o[at : at + count])
        mix = mixed[at : at + count]
        gn = gp[at : at + count] * key.astype(F32)
        ms = mix * scale
        gm = gains * scale * gn - mix * wide(coef_o[at : at + count])
        gc = (gm * query.astype(F32)).astype(BF)
        gc_o[at : at + count] = gc
        return ms, gn, gc.astype(F32)

    for at in range(0, ROWS, CHUNK):
        s = slice(at, at + CHUNK)
        ms, gn, gc = rows(at, CHUNK, qse[s], kmr[s])
        pm = (kmr[s].astype(F32) * (ms * gains)).astype(BF)
        xin[HALO + at : HALO + at + CHUNK] = pm
        g = rounded(up[s].astype(F32) * qmr[s].astype(F32))
        for step in range(7):
            sums[step] = sums[step] + eights(gc * prod[pl.ds(8 + at - step, CHUNK), :])
        sums[7] = sums[7] + eights(g * pm.astype(F32))
        sums[8] = sums[8] + eights(gn * ms)
    rows(ROWS, 8, bwd[HEAD : HEAD + 8], bwd[HEAD + 8 : HEAD + 16])
    parts = [jnp.sum(x, axis=0, keepdims=True) for x in sums]
    small[i] = jnp.concatenate(parts + [jnp.zeros((7, CB), F32)], 0)

    x = forward(fxh[...], fxl[...], xin[...])
    xspec[...] = x
    gl = gloc[...]
    xr, xi, gr, gi = x[:HALF], x[HALF:], gl[:HALF], gl[HALF:]
    back = jnp.concatenate([gr * xr + gi * xi, gi * xr - gr * xi], 0)
    corr = inverse(th[...], tl[...], back).T.astype(BF)
    for zz in range(4):
        for yc in range(4):
            at = pl.multiple_of((4 * i + zz) * 16, 16)
            payload[yc, pl.ds(at, 16), :] = corr[zz * 64 + yc * 16 : zz * 64 + yc * 16 + 16]

    @pl.when(i == last)
    def _():
        lane = lax.broadcasted_iota(jnp.int32, (16, 128), 1)
        row = lax.broadcasted_iota(jnp.int32, (16, 128), 0)
        spread = (lane % 16 == row).astype(BF)
        chan = lax.broadcasted_iota(jnp.int32, (CB, 128), 0)
        keep = chan % 8 == lax.broadcasted_iota(jnp.int32, (CB, 128), 1) // 16
        out_row = lax.broadcasted_iota(jnp.int32, (128, CB), 0)
        out_chan = lax.broadcasted_iota(jnp.int32, (128, CB), 1)
        packed = None
        for block in range(4):
            tiled = lax.dot_general(
                small[block].astype(BF), spread, (((0,), (0,)), ((), ())), preferred_element_type=F32
            )
            masked = jnp.where(keep, tiled, 0.0).astype(BF)
            c = out_chan + block * CB
            take = (out_row // 32 == (c // 16) % 4) & ((out_row // 2) % 16 == c // 64) & (out_row % 2 == (c // 8) % 2)
            part = dot(take.astype(BF), masked)
            packed = part if packed is None else packed + part
        packed = packed.astype(BF)
        for yc in range(4):
            payload[yc, 256:] = packed[yc * 32 : yc * 32 + 32]


def rest_kernel(
    xspec, hspec, th, tl, up, kmr, mixed, conv, gp, gc, kse, vse, gain, skip, fse, scale, coef,
    gqse, gkse, gvse, gqmr, gkmr, ym, gcf
):
    x, h = xspec[...], hspec[...]
    xr, xi, hr, hi = x[:HALF], x[HALF:], h[:HALF], h[HALF:]
    spec = jnp.concatenate([xr * hr - xi * hi, xi * hr + xr * hi], 0)
    ym[...] = inverse(th[:ROWS], tl[:ROWS], spec)
    gcf[...] = gc[...].astype(F32)
    gains, taps = gain[...], fse[...]
    for at in range(0, ROWS, CHUNK):
        s = slice(at, at + CHUNK)
        sc = wide(scale[s])
        key = kmr[s].astype(F32)
        mix = mixed[s]
        grad = gp[s]
        normed = mix * sc * gains
        pm = rounded(key * normed)
        gqmr[s] = (up[s].astype(F32) * (ym[s] + skip[...] * pm)).astype(BF)
        gkmr[s] = (grad * normed).astype(BF)
        gm = gains * sc * (grad * key) - mix * wide(coef[s])
        gqse[s] = (gm * conv[s]).astype(BF)
        gps = short_adjoint(gcf, taps, at, CHUNK)
        gkse[s] = (gps * vse[s].astype(F32)).astype(BF)
        gvse[s] = (gps * kse[s].astype(F32)).astype(BF)


def merge_kernel(got, out):
    total = got[0].astype(F32)
    for k in range(1, 4):
        total = total + got[k].astype(F32)
    for z in range(16):
        out[z, :16] = total[z * 16 : z * 16 + 16].astype(BF)
        pair = total[256 + z * 2 : 256 + z * 2 + 2]
        out[z, 16:] = jnp.concatenate([pair, jnp.zeros((6, 128), F32)], 0).astype(BF)


def final_kernel(got, se_o, mr_o, skip_o, gain_o, *, factor):
    total = got[0].astype(F32)
    for k in range(1, 16):
        total = total + got[k].astype(F32)
    total = total * factor
    eye = (
        lax.broadcasted_iota(jnp.int32, (16, 16), 0) == lax.broadcasted_iota(jnp.int32, (16, 16), 1)
    ).astype(F32)
    mr_o[...] = lax.dot_general(
        total[:16], eye, (((0,), (0,)), ((), ())), precision=lax.Precision.HIGHEST, preferred_element_type=F32
    )
    chan = lax.broadcasted_iota(jnp.int32, (16, 128), 0)
    lane = lax.broadcasted_iota(jnp.int32, (16, 128), 1)
    mine = jnp.where(chan < 8, total[16:17], total[17:18])
    mine = jnp.where(lane // 16 == chan % 8, mine, 0.0)
    pick = (lane % 16 == chan).astype(F32)
    small = lax.dot_general(
        pick, mine, (((1,), (1,)), ((), ())), precision=lax.Precision.HIGHEST, preferred_element_type=F32
    )
    se_o[...] = small[:7]
    skip_o[...] = small[7:8]
    gain_o[...] = small[8:9]


def local(
    query_se, key_se, value_se, query_mr, key_mr, upstream, filter_se, filter_mr, skip_mr, norm_gain
):
    chans = query_se.shape[1]
    steps = chans // CB
    size = lax.axis_size("ctx")
    skip2, gain2 = skip_mr.reshape(1, chans), norm_gain.reshape(1, chans)
    fx = halves(basis(-HALO, ROWS))
    fhead = halves(basis(ROWS, ROWS + HEAD))
    back = halves(basis(0, EXT).T * (2.0 / LEN))

    def cols(rows):
        return pl.BlockSpec((rows, CB), lambda i: (0, i))

    def whole(*shape):
        return pl.BlockSpec(shape, lambda i: (0,) * len(shape))

    def shape(rows, dtype):
        return jax.ShapeDtypeStruct((rows, chans), dtype)

    params = pltpu.CompilerParams(dimension_semantics=("arbitrary",), vmem_limit_bytes=48 * 1024 * 1024)
    stream, one = cols(ROWS), cols(1)

    fwd, bwd = pl.pallas_call(
        send_kernel,
        grid=(steps,),
        in_specs=[stream] * 6 + [cols(7), one],
        out_specs=[cols(FWD), cols(BWD)],
        out_shape=[shape(FWD, BF), shape(BWD, BF)],
        scratch_shapes=[pltpu.VMEM((HALO + 16, CB), F32), pltpu.VMEM((HALO, 128), F32)],
        compiler_params=params,
        name="send",
    )(key_se, value_se, query_se, key_mr, upstream, query_mr, filter_se, gain2)

    down = [(k, k + 1) for k in range(size - 1)]
    upward = [(k + 1, k) for k in range(size - 1)]
    bwd = lax.ppermute(bwd, "ctx", upward)
    fwd = lax.ppermute(fwd, "ctx", down)

    spectrum = cols(LEN)
    gloc, hspec = pl.pallas_call(
        local_kernel,
        grid=(steps,),
        in_specs=[stream, stream, cols(128), whole(LEN, HALO + ROWS), whole(LEN, HALO + ROWS)],
        out_specs=[spectrum, spectrum],
        out_shape=[shape(LEN, F32), shape(LEN, F32)],
        compiler_params=params,
        name="local",
    )(upstream, query_mr, filter_mr, *fx)

    mixed, conv, gp, stats = pl.pallas_call(
        norm_kernel,
        grid=(steps,),
        in_specs=[cols(FWD), cols(BWD)] + [stream] * 6 + [cols(7), one, one, spectrum, spectrum]
        + [whole(LEN, HEAD)] * 2 + [whole(EXT, LEN)] * 2,
        out_specs=[cols(EXT), cols(EXT), cols(EXT), whole(8, 8, 128)],
        out_shape=[shape(EXT, F32), shape(EXT, F32), shape(EXT, F32), jax.ShapeDtypeStruct((8, 8, 128), F32)],
        scratch_shapes=[
            pltpu.VMEM((ROWS + 16, CB), F32), pltpu.VMEM((8, 128), F32),
            pltpu.VMEM((256, 128), F32), pltpu.VMEM((256, 128), F32),
        ],
        compiler_params=params,
        name="norm",
    )(fwd, bwd, key_se, value_se, query_se, key_mr, upstream, query_mr, filter_se, gain2, skip2, gloc, hspec,
      *fhead, *back)

    stats = lax.all_to_all(stats, "tp", 0, 0, tiled=True)

    payload, xspec, gc, scale, coef = pl.pallas_call(
        filter_kernel,
        grid=(steps,),
        in_specs=[whole(8, 8, 128), cols(FWD), cols(EXT), cols(EXT)] + [stream] * 6
        + [cols(BWD), one, spectrum] + [whole(LEN, HALO + ROWS)] * 2 + [whole(128, LEN)] * 2,
        out_specs=[whole(4, 288, 128), spectrum, cols(EXT), whole(EXT, 128), whole(EXT, 128)],
        out_shape=[jax.ShapeDtypeStruct((4, 288, 128), BF), shape(LEN, F32), shape(EXT, BF),
                   jax.ShapeDtypeStruct((EXT, 128), F32), jax.ShapeDtypeStruct((EXT, 128), F32)],
        scratch_shapes=[
            pltpu.VMEM((ROWS + 8, CB), F32), pltpu.VMEM((HALO, 128), F32),
            pltpu.VMEM((steps, 16, CB), F32), pltpu.VMEM((HALO + ROWS, CB), BF),
        ],
        compiler_params=params,
        name="filters",
    )(stats, fwd, mixed, gp, key_mr, query_se, upstream, query_mr, key_se, value_se, bwd, gain2, gloc, *fx, *back)

    near = [[4 * a + b for b in range(4)] for a in range(size // 4)]
    far = [[4 * a + b for a in range(size // 4)] for b in range(4)]
    got = lax.all_to_all(payload, "ctx", 0, 0, axis_index_groups=near, tiled=True)

    outs = pl.pallas_call(
        rest_kernel,
        grid=(steps,),
        in_specs=[spectrum, spectrum, whole(EXT, LEN), whole(EXT, LEN), stream, stream, cols(EXT), cols(EXT),
                  cols(EXT), cols(EXT), stream, stream, one, one, cols(7), whole(EXT, 128), whole(EXT, 128)],
        out_specs=[stream] * 5,
        out_shape=[shape(ROWS, BF)] * 5,
        scratch_shapes=[pltpu.VMEM((ROWS, CB), F32), pltpu.VMEM((EXT, CB), F32)],
        compiler_params=params,
        name="rest",
    )(xspec, hspec, *back, upstream, key_mr, mixed, conv, gp, gc, key_se, value_se, gain2, skip2, filter_se,
      scale, coef)

    merged = pl.pallas_call(
        merge_kernel, out_shape=jax.ShapeDtypeStruct((16, 24, 128), BF), name="merge"
    )(got)
    got = lax.all_to_all(merged, "ctx", 0, 0, axis_index_groups=far, tiled=True)
    factor = 1.0 / math.sqrt(ROWS * size)
    se, mr, sk, ga = pl.pallas_call(
        lambda *refs: final_kernel(*refs, factor=factor),
        out_shape=[jax.ShapeDtypeStruct((7, 16), F32), jax.ShapeDtypeStruct((128, 16), F32),
                   jax.ShapeDtypeStruct((1, 16), F32), jax.ShapeDtypeStruct((1, 16), F32)],
        name="final",
    )(got)
    return (*outs, se, mr, sk.reshape(16), ga.reshape(16))


def solution(mesh):
    both, part = P("ctx", "tp"), P(None, "tp")
    in_specs = (both,) * 6 + (part, part, P("tp"), P("tp"))
    split_all = ("tp", "ctx")
    out_specs = (both,) * 5 + (P(None, split_all), P(None, split_all), P(split_all), P(split_all))
    return jax.shard_map(local, mesh=mesh, in_specs=in_specs, out_specs=out_specs, check_vma=False)
```

```python
import math

import jax
import jax.numpy as jnp
import numpy as np
from jax import lax
from jax.experimental import pallas as pl
from jax.experimental.pallas import tpu as pltpu
from jax.sharding import PartitionSpec as P

D = 8192
EPSILON = 0.1
BF = jnp.bfloat16
F32 = jnp.float32

LEN = 384
HALF = LEN // 2
ROWS = 224
EXT = ROWS + 8
HALO = 128
HEAD = 136
CB = 256
FWD = HALO + 8 + 8
BWD = HEAD + 24
CHUNK = 32


def basis(first, last):
    theta = np.pi * (2 * np.arange(HALF)[:, None] + 1) / LEN * np.arange(first, last)[None, :]
    return np.concatenate([np.cos(theta), -np.sin(theta)], 0)


def halves(matrix):
    high = matrix.astype(BF)
    low = (matrix - high.astype(np.float64)).astype(BF)
    return high, low


def dot(a, b):
    return jnp.dot(a, b, preferred_element_type=F32)


def split(x):
    high = x.astype(BF)
    return high, (x - high.astype(F32)).astype(BF)


def forward(fh, fl, data):
    return dot(fh, data) + dot(fl, data)


def inverse(th, tl, spectrum):
    high, low = split(spectrum)
    return dot(th, high) + dot(tl, high) + dot(th, low)


def wide(column):
    return jnp.concatenate([column] * (CB // 128), axis=1)


def folded(x):
    total = x[:, :128]
    for at in range(128, x.shape[1], 128):
        total = total + x[:, at : at + 128]
    return total


def sums_in_lanes(acc):
    ones = jnp.ones((8, 128), F32)
    return lax.dot_general(
        ones, acc, (((1,), (1,)), ((), ())), precision=lax.Precision.HIGHEST, preferred_element_type=F32
    )


def short_conv(ref, taps, row, count):
    total = None
    for step in range(7):
        term = taps[step : step + 1, :] * ref[pl.ds(row - step, count), :]
        total = term if total is None else total + term
    return total


def short_adjoint(ref, taps, row, count):
    total = None
    for step in range(7):
        term = taps[step : step + 1, :] * ref[pl.ds(row + step, count), :]
        total = term if total is None else total + term
    return total


def rounded(x):
    return x.astype(BF).astype(F32)


def block(b):
    return pl.ds(pl.multiple_of(b * CB, CB), CB)


def eights(x):
    total = x[:8]
    for r in range(8, x.shape[0], 8):
        total = total + x[r : r + 8]
    return total


def send_kernel(
    kse, vse, qse, kmr, up, qmr, fse, gain, fwd, bwd,
    kse_t, vse_t, qse_t, kmr_t, up_h, qmr_h, kse_h, vse_h, qse_h, kmr_h, taps_v, gain_v, sems, prod, acc
):
    last = ROWS - HALO
    first = last - 16
    pieces = [
        (up.at[pl.ds(0, HEAD)], up_h), (qmr.at[pl.ds(0, HEAD)], qmr_h),
        (qse.at[pl.ds(0, 8)], qse_h), (kmr.at[pl.ds(0, 8)], kmr_h),
        (kse.at[pl.ds(0, 8)], kse_h), (vse.at[pl.ds(0, 8)], vse_h),
        (kse.at[pl.ds(first, HALO + 16)], kse_t), (vse.at[pl.ds(first, HALO + 16)], vse_t), (fse, taps_v),
        (qse.at[pl.ds(last, HALO)], qse_t), (kmr.at[pl.ds(last, HALO)], kmr_t), (gain, gain_v),
    ]
    copies = [pltpu.make_async_copy(src, dst, sems.at[k]) for k, (src, dst) in enumerate(pieces)]
    for copy in copies:
        copy.start()
    acc[...] = jnp.zeros_like(acc)
    fwd[HALO + 8 :] = jnp.zeros((8, fwd.shape[1]), BF)
    for copy in copies[:6]:
        copy.wait()

    def head(b, carry):
        c = block(b)
        bwd[:HEAD, c] = (up_h[:, c].astype(F32) * qmr_h[:, c].astype(F32)).astype(BF)
        bwd[HEAD : HEAD + 8, c] = qse_h[:, c]
        bwd[HEAD + 8 : HEAD + 16, c] = kmr_h[:, c]
        bwd[HEAD + 16 :, c] = (kse_h[:, c].astype(F32) * vse_h[:, c].astype(F32)).astype(BF)
        return carry

    lax.fori_loop(0, fwd.shape[1] // CB, head, 0)
    for copy in copies[6:]:
        copy.wait()

    def tail(b, carry):
        c = block(b)
        product = rounded(kse_t[:, c].astype(F32) * vse_t[:, c].astype(F32))
        prod[...] = product
        taps, gains = taps_v[:, c], gain_v[:, c]
        for r in range(0, HALO, CHUNK):
            conv = short_conv(prod, taps, 16 + r, CHUNK)
            mixed = qse_t[r : r + CHUNK, c].astype(F32) * conv
            fwd[r : r + CHUNK, c] = (kmr_t[r : r + CHUNK, c].astype(F32) * mixed * gains).astype(BF)
            acc[r : r + CHUNK] += folded(mixed * mixed)
        fwd[HALO : HALO + 8, c] = product[HALO + 8 :].astype(BF)
        return carry

    lax.fori_loop(0, fwd.shape[1] // CB, tail, 0)
    total = sums_in_lanes(acc[...])
    high = total.astype(BF).astype(F32)
    rows = lax.broadcasted_iota(jnp.int32, (8, 128), 0)
    fwd[HALO + 8 :, :128] = jnp.where(rows == 0, high, jnp.where(rows == 1, total - high, 0.0)).astype(BF)


def local_kernel(
    up, qmr, kse, vse, qse, fmr, fse, fxh, fxl, gloc, hspec, conv_o, mixed_o, acc_o, prod
):
    acc_o[...] = jnp.zeros_like(acc_o)
    prod[:8] = jnp.zeros((8, CB), F32)

    def step(b, carry):
        c = block(b)
        g = (up[:, c].astype(F32) * qmr[:, c].astype(F32)).astype(BF)
        gloc[:, c] = forward(fxh[:, HALO:], fxl[:, HALO:], g)
        high, low = split(fmr[:, c])
        fh = fxh[:, HALO : HALO + 128]
        hspec[:, c] = dot(fh, high) + dot(fxl[:, HALO : HALO + 128], high) + dot(fh, low)
        prod[8:] = rounded(kse[:, c].astype(F32) * vse[:, c].astype(F32))
        taps = fse[:, c]
        for at in range(0, ROWS, CHUNK):
            conv = short_conv(prod, taps, 8 + at, CHUNK)
            mixed = qse[at : at + CHUNK, c].astype(F32) * conv
            conv_o[at : at + CHUNK, c] = conv
            mixed_o[at : at + CHUNK, c] = mixed
            square = folded(mixed * mixed)
            if at == 0:
                acc_o[8:CHUNK] += square[8:]
            else:
                acc_o[at : at + CHUNK] += square
        return carry

    lax.fori_loop(0, up.shape[1] // CB, step, 0)


def norm_kernel(
    fwd, bwd, kse, vse, qse, kmr, up, qmr, fse, gain, skip, gloc, hspec, mixed, acc_in, fhh, th,
    gp_o, conv_e, mixed_e, stats, prod, acc_sq, acc_w
):
    acc_sq[...] = acc_in[...]
    acc_w[...] = jnp.zeros_like(acc_w)

    def step(b, carry):
        c = block(b)
        spec = gloc[:, c] + dot(fhh[...], bwd[:HEAD, c])
        h = hspec[:, c]
        gr, gi, hr, hi = spec[:HALF], spec[HALF:], h[:HALF], h[HALF:]
        back = jnp.concatenate([(gr * hr + gi * hi).astype(BF), (gi * hr - gr * hi).astype(BF)], 0)
        gp_o[:, c] = dot(th[...], back)
        taps, gains, skips = fse[:, c], gain[:, c], skip[:, c]
        prod[:8] = fwd[HALO : HALO + 8, c].astype(F32)
        prod[8:16] = rounded(kse[:8, c].astype(F32) * vse[:8, c].astype(F32))
        prod[16:24] = rounded(kse[ROWS - 8 :, c].astype(F32) * vse[ROWS - 8 :, c].astype(F32))
        prod[24:] = bwd[HEAD + 16 :, c].astype(F32)
        edges = []
        for k, query in ((0, qse[:8, c]), (1, bwd[HEAD : HEAD + 8, c])):
            conv = short_conv(prod, taps, 8 + 16 * k, 8)
            edge = query.astype(F32) * conv
            conv_e[8 * k : 8 * k + 8, c] = conv
            mixed_e[8 * k : 8 * k + 8, c] = edge
            edges.append(edge)
            at = ROWS * k
            acc_sq[at : at + 8] += folded(edge * edge)

        def rows(at, count, mix, key, g):
            gp = gp_o[at : at + count, c] + skips * g
            gp_o[at : at + count, c] = gp
            acc_w[at : at + count] += folded(gp * key.astype(F32) * gains * mix)

        for at in range(0, ROWS, CHUNK):
            s = slice(at, at + CHUNK)
            mix = mixed[s, c]
            if at == 0:
                mix = jnp.concatenate([edges[0], mix[8:]], 0)
            rows(at, CHUNK, mix, kmr[s, c], rounded(up[s, c].astype(F32) * qmr[s, c].astype(F32)))
        rows(ROWS, 8, edges[1], bwd[HEAD + 8 : HEAD + 16, c], bwd[:8, c].astype(F32))
        return carry

    lax.fori_loop(0, gloc.shape[1] // CB, step, 0)
    sq = sums_in_lanes(acc_sq[...])
    w = sums_in_lanes(acc_w[...])
    sent = fwd[HALO + 8 :, :128].astype(F32)
    mine = jnp.concatenate(
        [sq[:1, :128], sq[:1, 128:], w[:1, :128], w[:1, 128:], sent[:1] + sent[1:2], jnp.zeros((3, 128), F32)], 0
    )
    for dev in range(8):
        stats[dev] = mine


def column(total, row):
    pick = (lax.broadcasted_iota(jnp.int32, (8, 128), 0) == row).astype(F32)
    return lax.dot_general(
        total, pick, (((0,), (0,)), ((), ())), precision=lax.Precision.HIGHEST, preferred_element_type=F32
    )


def finish_kernel(
    stats, fwd, mixed, conv, mixed_e, conv_e, gp, kmr, qse, up, qmr, kse, vse, bwd, gain, skip, fse, gloc, hspec,
    fxh, th, gqse, gkse, gvse, gqmr, gkmr, payload,
    prod, scale_s, coef_s, halo_s, small, xin, gcf, o0, o1, o2, o3, o4, sems
):
    steps = gloc.shape[1] // CB
    total = stats[0]
    for dev in range(1, 8):
        total = total + stats[dev]
    s0 = lax.rsqrt(column(total, 0) / D + EPSILON)
    s1 = lax.rsqrt(column(total, 1) / D + EPSILON)
    scale_s[:128] = s0
    scale_s[128:] = s1
    coef_s[:128] = s0 * s0 * s0 * (column(total, 2) / D)
    coef_s[128:] = s1 * s1 * s1 * (column(total, 3) / D)
    halo_s[...] = lax.rsqrt(column(total, 4) / D + EPSILON)
    outs = ((o0, gqse), (o1, gkse), (o2, gvse), (o3, gqmr), (o4, gkmr))

    def out_copies(b):
        c = block(b)
        return [pltpu.make_async_copy(src.at[:, c], dst.at[:, c], sems.at[k, b]) for k, (src, dst) in enumerate(outs)]

    def step(b, carry):
        c = block(b)
        for at in range(0, HALO, CHUNK):
            s = slice(at, at + CHUNK)
            xin[s] = (fwd[s, c].astype(F32) * wide(halo_s[s])).astype(BF)
        prod[:8] = fwd[HALO : HALO + 8, c].astype(F32)
        prod[8:] = rounded(kse[:, c].astype(F32) * vse[:, c].astype(F32))
        gains, taps, skips = gain[:, c], fse[:, c], skip[:, c]
        sums = [jnp.zeros((8, CB), F32) for _ in range(9)]

        def mix_of(at, count):
            mix, con = mixed[at : at + count, c], conv[at : at + count, c]
            if at == 0:
                mix = jnp.concatenate([mixed_e[:8, c], mix[8:]], 0)
                con = jnp.concatenate([conv_e[:8, c], con[8:]], 0)
            return mix, con

        for at in range(0, ROWS, CHUNK):
            s = slice(at, at + CHUNK)
            mix, con = mix_of(at, CHUNK)
            scale = wide(scale_s[s])
            key = kmr[s, c].astype(F32)
            grad = gp[s, c]
            gn = grad * key
            ms = mix * scale
            normed = ms * gains
            gm = gains * scale * gn - mix * wide(coef_s[s])
            gc = rounded(gm * qse[s, c].astype(F32))
            gcf[s] = gc
            o0[s, c] = (gm * con).astype(BF)
            o4[s, c] = (grad * normed).astype(BF)
            pm = (key * normed).astype(BF)
            xin[HALO + at : HALO + at + CHUNK] = pm
            g = rounded(up[s, c].astype(F32) * qmr[s, c].astype(F32))
            for tap in range(7):
                sums[tap] = sums[tap] + eights(gc * prod[pl.ds(8 + at - tap, CHUNK), :])
            sums[7] = sums[7] + eights(g * pm.astype(F32))
            sums[8] = sums[8] + eights(gn * ms)
        nxt = slice(ROWS, ROWS + 8)
        gn = gp[nxt, c] * bwd[HEAD + 8 : HEAD + 16, c].astype(F32)
        gm = gains * wide(scale_s[nxt]) * gn - mixed_e[8:, c] * wide(coef_s[nxt])
        gcf[nxt] = rounded(gm * bwd[HEAD : HEAD + 8, c].astype(F32))
        parts = [jnp.sum(x, axis=0, keepdims=True) for x in sums]
        small[b] = jnp.concatenate(parts + [jnp.zeros((7, CB), F32)], 0)

        x = dot(fxh[...], xin[...])
        gl, h = gloc[:, c], hspec[:, c]
        xr, xi, gr, gi, hr, hi = x[:HALF], x[HALF:], gl[:HALF], gl[HALF:], h[:HALF], h[HALF:]
        back = jnp.concatenate([(gr * xr + gi * xi).astype(BF), (gi * xr - gr * xi).astype(BF)], 0)
        corr = dot(th[:128], back).T.astype(BF)
        for zz in range(4):
            for yc in range(4):
                at = pl.multiple_of((4 * b + zz) * 16, 16)
                payload[yc, pl.ds(at, 16), :] = corr[zz * 64 + yc * 16 : zz * 64 + yc * 16 + 16]
        spec = jnp.concatenate([(xr * hr - xi * hi).astype(BF), (xi * hr + xr * hi).astype(BF)], 0)
        ym = dot(th[:ROWS], spec)
        for at in range(0, ROWS, CHUNK):
            s = slice(at, at + CHUNK)
            pm = xin[HALO + at : HALO + at + CHUNK].astype(F32)
            o3[s, c] = (up[s, c].astype(F32) * (ym[s] + skips * pm)).astype(BF)
            gps = short_adjoint(gcf, taps, at, CHUNK)
            o1[s, c] = (gps * vse[s, c].astype(F32)).astype(BF)
            o2[s, c] = (gps * kse[s, c].astype(F32)).astype(BF)
        for copy in out_copies(b):
            copy.start()
        return carry

    lax.fori_loop(0, steps, step, 0)

    lane = lax.broadcasted_iota(jnp.int32, (16, 128), 1)
    row = lax.broadcasted_iota(jnp.int32, (16, 128), 0)
    spread = (lane % 16 == row).astype(BF)
    chan = lax.broadcasted_iota(jnp.int32, (CB, 128), 0)
    keep = chan % 8 == lax.broadcasted_iota(jnp.int32, (CB, 128), 1) // 16
    out_row = lax.broadcasted_iota(jnp.int32, (128, CB), 0)
    out_chan = lax.broadcasted_iota(jnp.int32, (128, CB), 1)
    packed = None
    for b in range(steps):
        tiled = lax.dot_general(
            small[b].astype(BF), spread, (((0,), (0,)), ((), ())), preferred_element_type=F32
        )
        masked = jnp.where(keep, tiled, 0.0).astype(BF)
        ch = out_chan + b * CB
        take = (out_row // 32 == (ch // 16) % 4) & ((out_row // 2) % 16 == ch // 64) & (out_row % 2 == (ch // 8) % 2)
        part = dot(take.astype(BF), masked)
        packed = part if packed is None else packed + part
    packed = packed.astype(BF)
    for yc in range(4):
        payload[yc, 256:] = packed[yc * 32 : yc * 32 + 32]
    for b in range(steps):
        for copy in out_copies(b):
            copy.wait()


def merge_kernel(got, out):
    total = got[0].astype(F32)
    for k in range(1, 4):
        total = total + got[k].astype(F32)
    for z in range(16):
        out[z, :16] = total[z * 16 : z * 16 + 16].astype(BF)
        pair = total[256 + z * 2 : 256 + z * 2 + 2]
        out[z, 16:] = jnp.concatenate([pair, jnp.zeros((6, 128), F32)], 0).astype(BF)


def final_kernel(got, se_o, mr_o, skip_o, gain_o, *, factor):
    total = got[0].astype(F32)
    for k in range(1, 16):
        total = total + got[k].astype(F32)
    total = total * factor
    mr_o[...] = total[:16]
    chan = lax.broadcasted_iota(jnp.int32, (16, 128), 0)
    lane = lax.broadcasted_iota(jnp.int32, (16, 128), 1)
    mine = jnp.where(chan < 8, total[16:17], total[17:18])
    mine = jnp.where(lane // 16 == chan % 8, mine, 0.0)
    pick = (lane % 16 == chan).astype(F32)
    small = lax.dot_general(
        pick, mine, (((1,), (1,)), ((), ())), precision=lax.Precision.HIGHEST, preferred_element_type=F32
    )
    se_o[...] = small[:7]
    skip_o[...] = small[7:8]
    gain_o[...] = small[8:9]


def local(
    query_se, key_se, value_se, query_mr, key_mr, upstream, filter_se, filter_mr, skip_mr, norm_gain
):
    chans = query_se.shape[1]
    steps = chans // CB
    size = lax.axis_size("ctx")
    skip2, gain2 = skip_mr.reshape(1, chans), norm_gain.reshape(1, chans)
    fxh, fxl = halves(basis(-HALO, ROWS))
    fhead, _ = halves(basis(ROWS, ROWS + HEAD))
    back, _ = halves(basis(0, EXT).T * (2.0 / LEN))

    def shape(rows, dtype):
        return jax.ShapeDtypeStruct((rows, chans), dtype)

    def vmem(rows, width, dtype):
        return pltpu.VMEM((rows, width), dtype)

    params = pltpu.CompilerParams(vmem_limit_bytes=16 * 1024 * 1024)
    hbm = pl.BlockSpec(memory_space=pltpu.HBM)
    sent = (key_se, value_se, query_se, key_mr, upstream, query_mr, filter_se, gain2)
    fwd, bwd = pl.pallas_call(
        send_kernel,
        in_specs=[hbm] * 8,
        out_shape=[shape(FWD, BF), shape(BWD, BF)],
        scratch_shapes=[vmem(HALO + 16, chans, BF)] * 2 + [vmem(HALO, chans, BF)] * 2 + [vmem(HEAD, chans, BF)] * 2
        + [vmem(8, chans, BF)] * 4 + [vmem(7, chans, F32), vmem(1, chans, F32), pltpu.SemaphoreType.DMA((12,)),
           vmem(HALO + 16, CB, F32), vmem(HALO, 128, F32)],
        compiler_params=params,
        name="send",
    )(*(pltpu.with_memory_space_constraint(x, pltpu.HBM) for x in sent))

    down = [(k, k + 1) for k in range(size - 1)]
    upward = [(k + 1, k) for k in range(size - 1)]
    bwd = lax.ppermute(bwd, "ctx", upward)
    fwd = lax.ppermute(fwd, "ctx", down)

    gloc, hspec, conv, mixed, acc = pl.pallas_call(
        local_kernel,
        out_shape=[shape(LEN, F32), shape(LEN, F32), shape(ROWS, F32), shape(ROWS, F32),
                   jax.ShapeDtypeStruct((256, 128), F32)],
        scratch_shapes=[vmem(ROWS + 8, CB, F32)],
        compiler_params=params,
        name="local",
    )(upstream, query_mr, key_se, value_se, query_se, filter_mr, filter_se, fxh, fxl)

    gp, conv_e, mixed_e, stats = pl.pallas_call(
        norm_kernel,
        out_shape=[shape(EXT, F32), shape(16, F32), shape(16, F32), jax.ShapeDtypeStruct((8, 8, 128), F32)],
        scratch_shapes=[vmem(32, CB, F32), vmem(256, 128, F32), vmem(256, 128, F32)],
        compiler_params=params,
        name="norm",
    )(fwd, bwd, key_se, value_se, query_se, key_mr, upstream, query_mr, filter_se, gain2, skip2, gloc, hspec,
      mixed, acc, fhead, back)

    stats = lax.all_to_all(stats, "tp", 0, 0, tiled=True)

    *outs, payload = pl.pallas_call(
        finish_kernel,
        out_specs=[hbm] * 5 + [pl.BlockSpec(memory_space=pltpu.VMEM)],
        out_shape=[shape(ROWS, BF)] * 5 + [jax.ShapeDtypeStruct((4, 288, 128), BF)],
        scratch_shapes=[
            vmem(ROWS + 8, CB, F32), vmem(256, 128, F32), vmem(256, 128, F32), vmem(HALO, 128, F32),
            pltpu.VMEM((steps, 16, CB), F32), vmem(HALO + ROWS, CB, BF), vmem(EXT, CB, F32),
        ] + [vmem(ROWS, chans, BF)] * 5 + [pltpu.SemaphoreType.DMA((5, steps))],
        compiler_params=params,
        name="finish",
    )(stats, fwd, mixed, conv, mixed_e, conv_e, gp, key_mr, query_se, upstream, query_mr, key_se, value_se, bwd,
      gain2, skip2, filter_se, gloc, hspec, fxh, back)

    near = [[4 * a + b for b in range(4)] for a in range(size // 4)]
    far = [[4 * a + b for a in range(size // 4)] for b in range(4)]
    got = lax.all_to_all(payload, "ctx", 0, 0, axis_index_groups=near, tiled=True)
    merged = pl.pallas_call(
        merge_kernel, out_shape=jax.ShapeDtypeStruct((16, 24, 128), BF), compiler_params=params, name="merge"
    )(got)
    got = lax.all_to_all(merged, "ctx", 0, 0, axis_index_groups=far, tiled=True)
    factor = 1.0 / math.sqrt(ROWS * size)
    se, mr, sk, ga = pl.pallas_call(
        lambda *refs: final_kernel(*refs, factor=factor),
        out_shape=[jax.ShapeDtypeStruct((7, 16), F32), jax.ShapeDtypeStruct((16, 128), F32),
                   jax.ShapeDtypeStruct((1, 16), F32), jax.ShapeDtypeStruct((1, 16), F32)],
        compiler_params=params,
        name="final",
    )(got)
    return (*outs, se, mr.T, sk.reshape(16), ga.reshape(16))


def solution(mesh):
    both, part = P("ctx", "tp"), P(None, "tp")
    in_specs = (both,) * 6 + (part, part, P("tp"), P("tp"))
    split_all = ("tp", "ctx")
    out_specs = (both,) * 5 + (P(None, split_all), P(None, split_all), P(split_all), P(split_all))
    return jax.shard_map(local, mesh=mesh, in_specs=in_specs, out_specs=out_specs, check_vma=False)
```

```python
import math

import jax
import jax.numpy as jnp
import numpy as np
from jax import lax
from jax.experimental import pallas as pl
from jax.experimental.pallas import tpu as pltpu
from jax.sharding import PartitionSpec as P

D = 8192
EPSILON = 0.1
BF = jnp.bfloat16
F32 = jnp.float32

LEN = 384
HALF = LEN // 2
ROWS = 224
EXT = ROWS + 8
HALO = 128
HEAD = 136
CB = 256
BWD = HEAD + 24
CHUNK = 32


def basis(first, last):
    theta = np.pi * (2 * np.arange(HALF)[:, None] + 1) / LEN * np.arange(first, last)[None, :]
    return np.concatenate([np.cos(theta), -np.sin(theta)], 0)


def halves(matrix):
    high = matrix.astype(BF)
    low = (matrix - high.astype(np.float64)).astype(BF)
    return high, low


def dot(a, b):
    return jnp.dot(a, b, preferred_element_type=F32)


def split(x):
    high = x.astype(BF)
    return high, (x - high.astype(F32)).astype(BF)


def forward(fh, fl, data):
    return dot(fh, data) + dot(fl, data)


def wide(column):
    return jnp.concatenate([column] * (CB // 128), axis=1)


def folded(x):
    total = x[:, :128]
    for at in range(128, x.shape[1], 128):
        total = total + x[:, at : at + 128]
    return total


def sums_in_lanes(acc):
    ones = jnp.ones((8, 128), F32)
    return lax.dot_general(
        ones, acc, (((1,), (1,)), ((), ())), precision=lax.Precision.HIGHEST, preferred_element_type=F32
    )


def short_conv(ref, taps, row, count):
    total = None
    for step in range(7):
        term = taps[step : step + 1, :] * ref[pl.ds(row - step, count), :]
        total = term if total is None else total + term
    return total


def rounded(x):
    return x.astype(BF).astype(F32)


def block(b):
    return pl.ds(pl.multiple_of(b * CB, CB), CB)


def eights(x):
    total = x[:8]
    for r in range(8, x.shape[0], 8):
        total = total + x[r : r + 8]
    return total


def send_kernel(
    kse, vse, qse, kmr, up, qmr, fwd, bwd, up_h, qmr_h, kse_h, vse_h, qse_h, kmr_h, kse_t, vse_t, sems
):
    tail = pl.ds(ROWS - 8, 8)
    head = pl.ds(0, 8)
    pieces = [
        (up.at[pl.ds(0, HEAD)], up_h), (qmr.at[pl.ds(0, HEAD)], qmr_h), (qse.at[head], qse_h), (kmr.at[head], kmr_h),
        (kse.at[head], kse_h), (vse.at[head], vse_h), (kse.at[tail], kse_t), (vse.at[tail], vse_t),
    ]
    copies = [pltpu.make_async_copy(src, dst, sems.at[k]) for k, (src, dst) in enumerate(pieces)]
    for copy in copies:
        copy.start()
    for copy in copies:
        copy.wait()

    def step(b, carry):
        c = block(b)
        bwd[:HEAD, c] = (up_h[:, c].astype(F32) * qmr_h[:, c].astype(F32)).astype(BF)
        bwd[HEAD : HEAD + 8, c] = qse_h[:, c]
        bwd[HEAD + 8 : HEAD + 16, c] = kmr_h[:, c]
        bwd[HEAD + 16 :, c] = (kse_h[:, c].astype(F32) * vse_h[:, c].astype(F32)).astype(BF)
        fwd[:, c] = (kse_t[:, c].astype(F32) * vse_t[:, c].astype(F32)).astype(BF)
        return carry

    lax.fori_loop(0, fwd.shape[1] // CB, step, 0)


def local_kernel(
    up, qmr, kse, vse, qse, fse, fmr_in, fxh_in, fxl_in, gloc, hspec, conv_o, mixed_o, acc_o,
    prod, fmr, fxh, fxl, sems
):
    pieces = ((fmr_in, fmr), (fxh_in, fxh), (fxl_in, fxl))
    copies = [pltpu.make_async_copy(src, dst, sems.at[k]) for k, (src, dst) in enumerate(pieces)]
    for copy in copies:
        copy.start()
    acc_o[...] = jnp.zeros_like(acc_o)
    prod[:8] = jnp.zeros((8, CB), F32)
    steps = up.shape[1] // CB

    def short(b, carry):
        c = block(b)
        prod[8:] = rounded(kse[:, c].astype(F32) * vse[:, c].astype(F32))
        taps = fse[:, c]
        for at in range(0, ROWS, CHUNK):
            conv = short_conv(prod, taps, 8 + at, CHUNK)
            mixed = qse[at : at + CHUNK, c].astype(F32) * conv
            conv_o[at : at + CHUNK, c] = conv
            mixed_o[at : at + CHUNK, c] = mixed
            square = folded(mixed * mixed)
            if at == 0:
                acc_o[8:CHUNK] += square[8:]
            else:
                acc_o[at : at + CHUNK] += square
        return carry

    lax.fori_loop(0, steps, short, 0)
    for copy in copies:
        copy.wait()

    def spectra(b, carry):
        c = block(b)
        g = (up[:, c].astype(F32) * qmr[:, c].astype(F32)).astype(BF)
        gloc[:, c] = forward(fxh[...], fxl[...], g)
        high, low = split(fmr[:, c])
        fh = fxh[:, :128]
        hspec[:, c] = dot(fh, high) + dot(fxl[:, :128], high) + dot(fh, low)
        return carry

    lax.fori_loop(0, steps, spectra, 0)


def norm_kernel(
    fwd, bwd, kse, vse, qse, kmr, up, qmr, fse, gain, skip, gloc, hspec, mixed, acc_in, fhh, th,
    gp_o, gext_o, conv_e, mixed_e, stats, prod, acc_sq, acc_w
):
    acc_sq[...] = acc_in[...]
    acc_w[...] = jnp.zeros_like(acc_w)

    def step(b, carry):
        c = block(b)
        spec = gloc[:, c] + dot(fhh[...], bwd[:HEAD, c])
        gext_o[:, c] = spec
        h = hspec[:, c]
        gr, gi, hr, hi = spec[:HALF], spec[HALF:], h[:HALF], h[HALF:]
        back = jnp.concatenate([(gr * hr + gi * hi).astype(BF), (gi * hr - gr * hi).astype(BF)], 0)
        gp_o[:, c] = dot(th[...], back)
        taps, gains, skips = fse[:, c], gain[:, c], skip[:, c]
        prod[:8] = fwd[:, c].astype(F32)
        prod[8:16] = rounded(kse[:8, c].astype(F32) * vse[:8, c].astype(F32))
        prod[16:24] = rounded(kse[ROWS - 8 :, c].astype(F32) * vse[ROWS - 8 :, c].astype(F32))
        prod[24:] = bwd[HEAD + 16 :, c].astype(F32)
        edges = []
        for k, query in ((0, qse[:8, c]), (1, bwd[HEAD : HEAD + 8, c])):
            conv = short_conv(prod, taps, 8 + 16 * k, 8)
            edge = query.astype(F32) * conv
            conv_e[8 * k : 8 * k + 8, c] = conv
            mixed_e[8 * k : 8 * k + 8, c] = edge
            edges.append(edge)
            at = ROWS * k
            acc_sq[at : at + 8] += folded(edge * edge)

        def rows(at, count, mix, key, g):
            gp = gp_o[at : at + count, c] + skips * g
            gp_o[at : at + count, c] = gp
            acc_w[at : at + count] += folded(gp * key.astype(F32) * gains * mix)

        for at in range(0, ROWS, CHUNK):
            s = slice(at, at + CHUNK)
            mix = mixed[s, c]
            if at == 0:
                mix = jnp.concatenate([edges[0], mix[8:]], 0)
            rows(at, CHUNK, mix, kmr[s, c], rounded(up[s, c].astype(F32) * qmr[s, c].astype(F32)))
        rows(ROWS, 8, edges[1], bwd[HEAD + 8 : HEAD + 16, c], bwd[:8, c].astype(F32))
        return carry

    lax.fori_loop(0, gloc.shape[1] // CB, step, 0)
    sq = sums_in_lanes(acc_sq[...])
    w = sums_in_lanes(acc_w[...])
    mine = jnp.concatenate([sq[:1, :128], sq[:1, 128:], w[:1, :128], w[:1, 128:], jnp.zeros((4, 128), F32)], 0)
    for dev in range(8):
        stats[dev] = mine


def column(total, row):
    pick = (lax.broadcasted_iota(jnp.int32, (8, 128), 0) == row).astype(F32)
    return lax.dot_general(
        total, pick, (((0,), (0,)), ((), ())), precision=lax.Precision.HIGHEST, preferred_element_type=F32
    )


def merged_rows(body, edge, at, count, c=slice(None)):
    rows = body[at : at + count, c]
    return jnp.concatenate([edge[:8, c], rows[8:]], 0) if at == 0 else rows


def scales(stats, scale_s, coef_s):
    total = stats[0]
    for dev in range(1, 8):
        total = total + stats[dev]
    s0 = lax.rsqrt(column(total, 0) / D + EPSILON)
    s1 = lax.rsqrt(column(total, 1) / D + EPSILON)
    scale_s[:128] = s0
    scale_s[128:] = s1
    coef_s[:128] = s0 * s0 * s0 * (column(total, 2) / D)
    coef_s[128:] = s1 * s1 * s1 * (column(total, 3) / D)


def filter_kernel(
    stats, fwd, mixed, mixed_e, gp, kmr, qse, up, qmr, kse, vse, gain, gext, fxh, th,
    payload, halo, prod, small, scale_s, coef_s, pms
):
    steps = gext.shape[1] // CB
    scales(stats, scale_s, coef_s)

    def step(b, carry):
        c = block(b)
        prod[:8] = fwd[:, c].astype(F32)
        prod[8:] = rounded(kse[:, c].astype(F32) * vse[:, c].astype(F32))
        gains = gain[:, c]
        sums = [jnp.zeros((8, CB), F32) for _ in range(9)]
        for at in range(0, ROWS, CHUNK):
            s = slice(at, at + CHUNK)
            mix = merged_rows(mixed, mixed_e, at, CHUNK, c)
            scale = wide(scale_s[s])
            key = kmr[s, c].astype(F32)
            gn = gp[s, c] * key
            ms = mix * scale
            pm = (key * (ms * gains)).astype(BF)
            pms[s] = pm
            if at >= ROWS - HALO:
                halo[at - (ROWS - HALO) : at - (ROWS - HALO) + CHUNK, c] = pm
            gm = gains * scale * gn - mix * wide(coef_s[s])
            gc = rounded(gm * qse[s, c].astype(F32))
            g = rounded(up[s, c].astype(F32) * qmr[s, c].astype(F32))
            for tap in range(7):
                sums[tap] = sums[tap] + eights(gc * prod[pl.ds(8 + at - tap, CHUNK), :])
            sums[7] = sums[7] + eights(g * pm.astype(F32))
            sums[8] = sums[8] + eights(gn * ms)
        parts = [jnp.sum(x, axis=0, keepdims=True) for x in sums]
        small[b] = jnp.concatenate(parts + [jnp.zeros((7, CB), F32)], 0)

        x = dot(fxh[...], pms[...])
        ge = gext[:, c]
        xr, xi, gr, gi = x[:HALF], x[HALF:], ge[:HALF], ge[HALF:]
        back = jnp.concatenate([(gr * xr + gi * xi).astype(BF), (gi * xr - gr * xi).astype(BF)], 0)
        corr = dot(th[:128], back).T.astype(BF)
        for zz in range(4):
            for yc in range(4):
                at = pl.multiple_of((4 * b + zz) * 16, 16)
                payload[yc, pl.ds(at, 16), :] = corr[zz * 64 + yc * 16 : zz * 64 + yc * 16 + 16]
        return carry

    lax.fori_loop(0, steps, step, 0)

    lane = lax.broadcasted_iota(jnp.int32, (16, 128), 1)
    row = lax.broadcasted_iota(jnp.int32, (16, 128), 0)
    spread = (lane % 16 == row).astype(BF)
    chan = lax.broadcasted_iota(jnp.int32, (CB, 128), 0)
    keep = chan % 8 == lax.broadcasted_iota(jnp.int32, (CB, 128), 1) // 16
    out_row = lax.broadcasted_iota(jnp.int32, (128, CB), 0)
    out_chan = lax.broadcasted_iota(jnp.int32, (128, CB), 1)
    packed = None
    for b in range(steps):
        tiled = lax.dot_general(
            small[b].astype(BF), spread, (((0,), (0,)), ((), ())), preferred_element_type=F32
        )
        masked = jnp.where(keep, tiled, 0.0).astype(BF)
        ch = out_chan + b * CB
        take = (out_row // 32 == (ch // 16) % 4) & ((out_row // 2) % 16 == ch // 64) & (out_row % 2 == (ch // 8) % 2)
        part = dot(take.astype(BF), masked)
        packed = part if packed is None else packed + part
    packed = packed.astype(BF)
    for yc in range(4):
        payload[yc, 256:] = packed[yc * 32 : yc * 32 + 32]


def rest_kernel(
    stats, halo, hspec, mixed, conv, mixed_e, conv_e, gp, bwd, up, kmr, kse, vse, qse, gain, skip, fse, fxh, fhalo, th,
    gqse, gkse, gvse, gqmr, gkmr, scale_s, coef_s, gcs, pms
):
    @pl.when(pl.program_id(0) == 0)
    def _():
        scales(stats, scale_s, coef_s)

    gains, taps, skips = gain[...], fse[...], skip[...]
    for at in range(0, ROWS, CHUNK):
        s = slice(at, at + CHUNK)
        mix = merged_rows(mixed, mixed_e, at, CHUNK)
        con = merged_rows(conv, conv_e, at, CHUNK)
        scale, key, grad = wide(scale_s[s]), kmr[s].astype(F32), gp[s]
        normed = mix * scale * gains
        pms[s] = (key * normed).astype(BF)
        gkmr[s] = (grad * normed).astype(BF)
        gm = gains * scale * (grad * key) - mix * wide(coef_s[s])
        gqse[s] = (gm * con).astype(BF)
        gcs[s] = rounded(gm * qse[s].astype(F32))
    nxt = slice(ROWS, ROWS + 8)
    gn = gp[nxt] * bwd[HEAD + 8 : HEAD + 16].astype(F32)
    gm = gains * wide(scale_s[nxt]) * gn - mixed_e[8:] * wide(coef_s[nxt])
    gcs[nxt] = rounded(gm * bwd[HEAD : HEAD + 8].astype(F32))
    x, h = dot(fxh[...], pms[...]) + dot(fhalo[...], halo[...]), hspec[...]
    xr, xi, hr, hi = x[:HALF], x[HALF:], h[:HALF], h[HALF:]
    spec = jnp.concatenate([(xr * hr - xi * hi).astype(BF), (xi * hr + xr * hi).astype(BF)], 0)
    ym = dot(th[:ROWS], spec)
    for at in range(0, ROWS, CHUNK):
        s = slice(at, at + CHUNK)
        gqmr[s] = (up[s].astype(F32) * (ym[s] + skips * pms[s].astype(F32))).astype(BF)
        gps = None
        for tap in range(7):
            term = taps[tap : tap + 1, :] * gcs[pl.ds(at + tap, CHUNK), :]
            gps = term if gps is None else gps + term
        gkse[s] = (gps * vse[s].astype(F32)).astype(BF)
        gvse[s] = (gps * kse[s].astype(F32)).astype(BF)


def merge_kernel(got, out):
    total = got[0].astype(F32)
    for k in range(1, 4):
        total = total + got[k].astype(F32)
    for z in range(16):
        out[z, :16] = total[z * 16 : z * 16 + 16].astype(BF)
        pair = total[256 + z * 2 : 256 + z * 2 + 2]
        out[z, 16:] = jnp.concatenate([pair, jnp.zeros((6, 128), F32)], 0).astype(BF)


def final_kernel(got, se_o, mr_o, skip_o, gain_o, *, factor):
    total = got[0].astype(F32)
    for k in range(1, 16):
        total = total + got[k].astype(F32)
    total = total * factor
    mr_o[...] = total[:16]
    chan = lax.broadcasted_iota(jnp.int32, (16, 128), 0)
    lane = lax.broadcasted_iota(jnp.int32, (16, 128), 1)
    mine = jnp.where(chan < 8, total[16:17], total[17:18])
    mine = jnp.where(lane // 16 == chan % 8, mine, 0.0)
    pick = (lane % 16 == chan).astype(F32)
    small = lax.dot_general(
        pick, mine, (((1,), (1,)), ((), ())), precision=lax.Precision.HIGHEST, preferred_element_type=F32
    )
    se_o[...] = small[:7]
    skip_o[...] = small[7:8]
    gain_o[...] = small[8:9]


def local(
    query_se, key_se, value_se, query_mr, key_mr, upstream, filter_se, filter_mr, skip_mr, norm_gain
):
    chans = query_se.shape[1]
    steps = chans // CB
    size = lax.axis_size("ctx")
    skip2, gain2 = skip_mr.reshape(1, chans), norm_gain.reshape(1, chans)
    fxh, fxl = halves(basis(0, ROWS))
    fhead, _ = halves(basis(ROWS, ROWS + HEAD))
    fhalo, _ = halves(basis(-HALO, 0))
    back, _ = halves(basis(0, EXT).T * (2.0 / LEN))

    def shape(rows, dtype):
        return jax.ShapeDtypeStruct((rows, chans), dtype)

    def vmem(rows, width, dtype):
        return pltpu.VMEM((rows, width), dtype)

    def kept(x):
        return pltpu.with_memory_space_constraint(x, pltpu.HBM)

    params = pltpu.CompilerParams(vmem_limit_bytes=16 * 1024 * 1024)
    hbm = pl.BlockSpec(memory_space=pltpu.HBM)
    here = pl.BlockSpec(memory_space=pltpu.VMEM)
    fwd, bwd = pl.pallas_call(
        send_kernel,
        in_specs=[hbm] * 6,
        out_shape=[shape(8, BF), shape(BWD, BF)],
        scratch_shapes=[vmem(HEAD, chans, BF)] * 2 + [vmem(8, chans, BF)] * 6 + [pltpu.SemaphoreType.DMA((8,))],
        compiler_params=params,
        name="send",
    )(*(kept(x) for x in (key_se, value_se, query_se, key_mr, upstream, query_mr)))

    down = [(k, k + 1) for k in range(size - 1)]
    upward = [(k + 1, k) for k in range(size - 1)]
    bwd = lax.ppermute(bwd, "ctx", upward)
    fwd = lax.ppermute(fwd, "ctx", down)

    gloc, hspec, conv, mixed, acc = pl.pallas_call(
        local_kernel,
        in_specs=[here] * 6 + [hbm] * 3,
        out_shape=[shape(LEN, F32), shape(LEN, F32), shape(ROWS, F32), shape(ROWS, F32),
                   jax.ShapeDtypeStruct((256, 128), F32)],
        scratch_shapes=[vmem(ROWS + 8, CB, F32), vmem(filter_mr.shape[0], chans, F32), vmem(LEN, ROWS, BF),
                        vmem(LEN, ROWS, BF), pltpu.SemaphoreType.DMA((3,))],
        compiler_params=params,
        name="local",
    )(upstream, query_mr, key_se, value_se, query_se, filter_se, kept(filter_mr), kept(fxh), kept(fxl))

    gp, gext, conv_e, mixed_e, stats = pl.pallas_call(
        norm_kernel,
        out_shape=[shape(EXT, F32), shape(LEN, F32), shape(16, F32), shape(16, F32),
                   jax.ShapeDtypeStruct((8, 8, 128), F32)],
        scratch_shapes=[vmem(32, CB, F32), vmem(256, 128, F32), vmem(256, 128, F32)],
        compiler_params=params,
        name="norm",
    )(fwd, bwd, key_se, value_se, query_se, key_mr, upstream, query_mr, filter_se, gain2, skip2, gloc, hspec,
      mixed, acc, fhead, back)

    stats = lax.all_to_all(stats, "tp", 0, 0, tiled=True)

    payload, halo = pl.pallas_call(
        filter_kernel,
        out_shape=[jax.ShapeDtypeStruct((4, 288, 128), BF), shape(HALO, BF)],
        scratch_shapes=[vmem(ROWS + 8, CB, F32), pltpu.VMEM((steps, 16, CB), F32), vmem(256, 128, F32),
                        vmem(256, 128, F32), vmem(ROWS, CB, BF)],
        compiler_params=params,
        name="filters",
    )(stats, fwd, mixed, mixed_e, gp, key_mr, query_se, upstream, query_mr, key_se, value_se, gain2, gext, fxh, back)
    halo = lax.ppermute(halo, "ctx", down)

    def cols(rows):
        return pl.BlockSpec((rows, CB), lambda i: (0, i))

    def whole(*dims):
        return pl.BlockSpec(dims, lambda i: (0,) * len(dims))

    late = (stats, halo, hspec, mixed, conv, mixed_e, conv_e, gp, bwd, upstream, key_mr, key_se, value_se, query_se,
            gain2, skip2, filter_se, fxh, fhalo, back)
    outs = pl.pallas_call(
        rest_kernel,
        grid=(steps,),
        in_specs=[whole(8, 8, 128)] + [cols(x.shape[0]) for x in late[1:17]] + [whole(*x.shape) for x in late[17:]],
        out_specs=[cols(ROWS)] * 5,
        out_shape=[shape(ROWS, BF)] * 5,
        scratch_shapes=[vmem(256, 128, F32), vmem(256, 128, F32), vmem(EXT, CB, F32), vmem(ROWS, CB, BF)],
        compiler_params=params,
        name="rest",
    )(*(kept(x) for x in late))

    near = [[4 * a + b for b in range(4)] for a in range(size // 4)]
    far = [[4 * a + b for a in range(size // 4)] for b in range(4)]
    got = lax.all_to_all(payload, "ctx", 0, 0, axis_index_groups=near, tiled=True)
    merged = pl.pallas_call(
        merge_kernel, out_shape=jax.ShapeDtypeStruct((16, 24, 128), BF), compiler_params=params, name="merge"
    )(got)
    got = lax.all_to_all(merged, "ctx", 0, 0, axis_index_groups=far, tiled=True)
    factor = 1.0 / math.sqrt(ROWS * size)
    se, mr, sk, ga = pl.pallas_call(
        lambda *refs: final_kernel(*refs, factor=factor),
        out_shape=[jax.ShapeDtypeStruct((7, 16), F32), jax.ShapeDtypeStruct((16, 128), F32),
                   jax.ShapeDtypeStruct((1, 16), F32), jax.ShapeDtypeStruct((1, 16), F32)],
        compiler_params=params,
        name="final",
    )(got)
    return (*outs, se, mr.T, sk.reshape(16), ga.reshape(16))


def solution(mesh):
    both, part = P("ctx", "tp"), P(None, "tp")
    in_specs = (both,) * 6 + (part, part, P("tp"), P("tp"))
    split_all = ("tp", "ctx")
    out_specs = (both,) * 5 + (P(None, split_all), P(None, split_all), P(split_all), P(split_all))
    return jax.shard_map(local, mesh=mesh, in_specs=in_specs, out_specs=out_specs, check_vma=False)
```

```python
import math

import jax
import jax.numpy as jnp
import numpy as np
from jax import lax
from jax.experimental import pallas as pl
from jax.experimental.pallas import tpu as pltpu
from jax.sharding import PartitionSpec as P

D = 8192
EPSILON = 0.1
BF = jnp.bfloat16
F32 = jnp.float32

LEN = 384
HALF = LEN // 2
ROWS = 224
EXT = ROWS + 8
HALO = 128
HEAD = 136
CB = 256
BWD = HEAD + 24
CHUNK = 32


def basis(first, last):
    theta = np.pi * (2 * np.arange(HALF)[:, None] + 1) / LEN * np.arange(first, last)[None, :]
    return np.concatenate([np.cos(theta), -np.sin(theta)], 0)


def halves(matrix):
    high = matrix.astype(BF)
    low = (matrix - high.astype(np.float64)).astype(BF)
    return high, low


def dot(a, b):
    return jnp.dot(a, b, preferred_element_type=F32)


def split(x):
    high = x.astype(BF)
    return high, (x - high.astype(F32)).astype(BF)


def forward(fh, fl, data):
    return dot(fh, data) + dot(fl, data)


def wide(column):
    return jnp.concatenate([column] * (CB // 128), axis=1)


def folded(x):
    total = x[:, :128]
    for at in range(128, x.shape[1], 128):
        total = total + x[:, at : at + 128]
    return total


def sums_in_lanes(acc):
    ones = jnp.ones((8, 128), F32)
    return lax.dot_general(
        ones, acc, (((1,), (1,)), ((), ())), precision=lax.Precision.HIGHEST, preferred_element_type=F32
    )


def short_conv(ref, taps, row, count):
    total = None
    for step in range(7):
        term = taps[step : step + 1, :] * ref[pl.ds(row - step, count), :]
        total = term if total is None else total + term
    return total


def short_adjoint(ref, taps, row, count):
    total = None
    for step in range(7):
        term = taps[step : step + 1, :] * ref[pl.ds(row + step, count), :]
        total = term if total is None else total + term
    return total


def rounded(x):
    return x.astype(BF).astype(F32)


def block(b):
    return pl.ds(pl.multiple_of(b * CB, CB), CB)


def eights(x):
    total = x[:8]
    for r in range(8, x.shape[0], 8):
        total = total + x[r : r + 8]
    return total


def send_kernel(
    kse, vse, qse, kmr, up, qmr, fwd, bwd, up_h, qmr_h, kse_h, vse_h, qse_h, kmr_h, kse_t, vse_t, sems
):
    tail = pl.ds(ROWS - 8, 8)
    head = pl.ds(0, 8)
    pieces = [
        (up.at[pl.ds(0, HEAD)], up_h), (qmr.at[pl.ds(0, HEAD)], qmr_h), (qse.at[head], qse_h), (kmr.at[head], kmr_h),
        (kse.at[head], kse_h), (vse.at[head], vse_h), (kse.at[tail], kse_t), (vse.at[tail], vse_t),
    ]
    copies = [pltpu.make_async_copy(src, dst, sems.at[k]) for k, (src, dst) in enumerate(pieces)]
    for copy in copies:
        copy.start()
    for copy in copies:
        copy.wait()

    def step(b, carry):
        c = block(b)
        bwd[:HEAD, c] = (up_h[:, c].astype(F32) * qmr_h[:, c].astype(F32)).astype(BF)
        bwd[HEAD : HEAD + 8, c] = qse_h[:, c]
        bwd[HEAD + 8 : HEAD + 16, c] = kmr_h[:, c]
        bwd[HEAD + 16 :, c] = (kse_h[:, c].astype(F32) * vse_h[:, c].astype(F32)).astype(BF)
        fwd[:, c] = (kse_t[:, c].astype(F32) * vse_t[:, c].astype(F32)).astype(BF)
        return carry

    lax.fori_loop(0, fwd.shape[1] // CB, step, 0)


def local_kernel(
    up, qmr, kse, vse, qse, fse, fmr_in, fxh_in, fxl_in, gloc, hspec, conv_o, mixed_o, acc_o,
    prod, fmr, fxh, fxl, sems
):
    pieces = ((fmr_in, fmr), (fxh_in, fxh), (fxl_in, fxl))
    copies = [pltpu.make_async_copy(src, dst, sems.at[k]) for k, (src, dst) in enumerate(pieces)]
    for copy in copies:
        copy.start()
    acc_o[...] = jnp.zeros_like(acc_o)
    prod[:8] = jnp.zeros((8, CB), F32)
    steps = up.shape[1] // CB

    def short(b, carry):
        c = block(b)
        prod[8:] = rounded(kse[:, c].astype(F32) * vse[:, c].astype(F32))
        taps = fse[:, c]
        for at in range(0, ROWS, CHUNK):
            conv = short_conv(prod, taps, 8 + at, CHUNK)
            mixed = qse[at : at + CHUNK, c].astype(F32) * conv
            conv_o[at : at + CHUNK, c] = conv
            mixed_o[at : at + CHUNK, c] = mixed
            square = folded(mixed * mixed)
            if at == 0:
                acc_o[8:CHUNK] += square[8:]
            else:
                acc_o[at : at + CHUNK] += square
        return carry

    lax.fori_loop(0, steps, short, 0)
    for copy in copies:
        copy.wait()

    def spectra(b, carry):
        c = block(b)
        g = (up[:, c].astype(F32) * qmr[:, c].astype(F32)).astype(BF)
        gloc[:, c] = forward(fxh[...], fxl[...], g)
        high, low = split(fmr[:, c])
        fh = fxh[:, :128]
        hspec[:, c] = dot(fh, high) + dot(fxl[:, :128], high) + dot(fh, low)
        return carry

    lax.fori_loop(0, steps, spectra, 0)


def norm_kernel(
    fwd, bwd, kse, vse, qse, kmr, up, qmr, fse, gain, skip, gloc, hspec, mixed, acc_in, fhh, th,
    gp_o, gext_o, conv_e, mixed_e, stats, prod, acc_sq, acc_w
):
    acc_sq[...] = acc_in[...]
    acc_w[...] = jnp.zeros_like(acc_w)

    def step(b, carry):
        c = block(b)
        spec = gloc[:, c] + dot(fhh[...], bwd[:HEAD, c])
        gext_o[:, c] = spec
        h = hspec[:, c]
        gr, gi, hr, hi = spec[:HALF], spec[HALF:], h[:HALF], h[HALF:]
        back = jnp.concatenate([(gr * hr + gi * hi).astype(BF), (gi * hr - gr * hi).astype(BF)], 0)
        gp_o[:, c] = dot(th[...], back)
        taps, gains, skips = fse[:, c], gain[:, c], skip[:, c]
        prod[:8] = fwd[:, c].astype(F32)
        prod[8:16] = rounded(kse[:8, c].astype(F32) * vse[:8, c].astype(F32))
        prod[16:24] = rounded(kse[ROWS - 8 :, c].astype(F32) * vse[ROWS - 8 :, c].astype(F32))
        prod[24:] = bwd[HEAD + 16 :, c].astype(F32)
        edges = []
        for k, query in ((0, qse[:8, c]), (1, bwd[HEAD : HEAD + 8, c])):
            conv = short_conv(prod, taps, 8 + 16 * k, 8)
            edge = query.astype(F32) * conv
            conv_e[8 * k : 8 * k + 8, c] = conv
            mixed_e[8 * k : 8 * k + 8, c] = edge
            edges.append(edge)
            at = ROWS * k
            acc_sq[at : at + 8] += folded(edge * edge)

        def rows(at, count, mix, key, g):
            gp = gp_o[at : at + count, c] + skips * g
            gp_o[at : at + count, c] = gp
            acc_w[at : at + count] += folded(gp * key.astype(F32) * gains * mix)

        for at in range(0, ROWS, CHUNK):
            s = slice(at, at + CHUNK)
            mix = mixed[s, c]
            if at == 0:
                mix = jnp.concatenate([edges[0], mix[8:]], 0)
            rows(at, CHUNK, mix, kmr[s, c], rounded(up[s, c].astype(F32) * qmr[s, c].astype(F32)))
        rows(ROWS, 8, edges[1], bwd[HEAD + 8 : HEAD + 16, c], bwd[:8, c].astype(F32))
        return carry

    lax.fori_loop(0, gloc.shape[1] // CB, step, 0)
    sq = sums_in_lanes(acc_sq[...])
    w = sums_in_lanes(acc_w[...])
    mine = jnp.concatenate([sq[:1, :128], sq[:1, 128:], w[:1, :128], w[:1, 128:], jnp.zeros((4, 128), F32)], 0)
    for dev in range(8):
        stats[dev] = mine


def column(total, row):
    pick = (lax.broadcasted_iota(jnp.int32, (8, 128), 0) == row).astype(F32)
    return lax.dot_general(
        total, pick, (((0,), (0,)), ((), ())), precision=lax.Precision.HIGHEST, preferred_element_type=F32
    )


def merged_rows(body, edge, at, count, c=slice(None)):
    rows = body[at : at + count, c]
    return jnp.concatenate([edge[:8, c], rows[8:]], 0) if at == 0 else rows


def scales(stats, scale_s, coef_s):
    total = stats[0]
    for dev in range(1, 8):
        total = total + stats[dev]
    s0 = lax.rsqrt(column(total, 0) / D + EPSILON)
    s1 = lax.rsqrt(column(total, 1) / D + EPSILON)
    scale_s[:128] = s0
    scale_s[128:] = s1
    coef_s[:128] = s0 * s0 * s0 * (column(total, 2) / D)
    coef_s[128:] = s1 * s1 * s1 * (column(total, 3) / D)


def filter_kernel(
    stats, fwd, bwd, mixed, mixed_e, conv, conv_e, gp, kmr, qse, up, qmr, kse, vse, gain, fse, gext, fxh, th,
    gqse, gkse, gvse, gkmr, pm_o, payload, halo, prod, small, scale_s, coef_s, gcs, o0, o1, o2, o3, pms, sems
):
    steps = gext.shape[1] // CB
    scales(stats, scale_s, coef_s)
    outs = ((pms, pm_o), (o0, gqse), (o3, gkmr), (o1, gkse), (o2, gvse))

    def out_copies(b):
        c = block(b)
        return [pltpu.make_async_copy(src.at[:, c], dst.at[:, c], sems.at[k, b]) for k, (src, dst) in enumerate(outs)]

    def step(b, carry):
        c = block(b)
        prod[:8] = fwd[:, c].astype(F32)
        prod[8:] = rounded(kse[:, c].astype(F32) * vse[:, c].astype(F32))
        gains = gain[:, c]
        sums = [jnp.zeros((8, CB), F32) for _ in range(9)]
        for at in range(0, ROWS, CHUNK):
            s = slice(at, at + CHUNK)
            mix = merged_rows(mixed, mixed_e, at, CHUNK, c)
            scale = wide(scale_s[s])
            key = kmr[s, c].astype(F32)
            grad = gp[s, c]
            gn = grad * key
            ms = mix * scale
            normed = ms * gains
            pm = (key * normed).astype(BF)
            pms[s, c] = pm
            o3[s, c] = (grad * normed).astype(BF)
            if at >= ROWS - HALO:
                halo[at - (ROWS - HALO) : at - (ROWS - HALO) + CHUNK, c] = pm
            gm = gains * scale * gn - mix * wide(coef_s[s])
            o0[s, c] = (gm * merged_rows(conv, conv_e, at, CHUNK, c)).astype(BF)
            gc = rounded(gm * qse[s, c].astype(F32))
            gcs[s] = gc
            g = rounded(up[s, c].astype(F32) * qmr[s, c].astype(F32))
            for tap in range(7):
                sums[tap] = sums[tap] + eights(gc * prod[pl.ds(8 + at - tap, CHUNK), :])
            sums[7] = sums[7] + eights(g * pm.astype(F32))
            sums[8] = sums[8] + eights(gn * ms)
        nxt = slice(ROWS, ROWS + 8)
        gn = gp[nxt, c] * bwd[HEAD + 8 : HEAD + 16, c].astype(F32)
        gm = gains * wide(scale_s[nxt]) * gn - mixed_e[8:, c] * wide(coef_s[nxt])
        gcs[nxt] = rounded(gm * bwd[HEAD : HEAD + 8, c].astype(F32))
        parts = [jnp.sum(x, axis=0, keepdims=True) for x in sums]
        small[b] = jnp.concatenate(parts + [jnp.zeros((7, CB), F32)], 0)

        x = dot(fxh[...], pms[:, c])
        ge = gext[:, c]
        xr, xi, gr, gi = x[:HALF], x[HALF:], ge[:HALF], ge[HALF:]
        back = jnp.concatenate([(gr * xr + gi * xi).astype(BF), (gi * xr - gr * xi).astype(BF)], 0)
        corr = dot(th[:128], back).T.astype(BF)
        for zz in range(4):
            for yc in range(4):
                at = pl.multiple_of((4 * b + zz) * 16, 16)
                payload[yc, pl.ds(at, 16), :] = corr[zz * 64 + yc * 16 : zz * 64 + yc * 16 + 16]
        taps = fse[:, c]
        for at in range(0, ROWS, CHUNK):
            s = slice(at, at + CHUNK)
            gps = short_adjoint(gcs, taps, at, CHUNK)
            o1[s, c] = (gps * vse[s, c].astype(F32)).astype(BF)
            o2[s, c] = (gps * kse[s, c].astype(F32)).astype(BF)
        for copy in out_copies(b):
            copy.start()
        return carry

    lax.fori_loop(0, steps, step, 0)

    lane = lax.broadcasted_iota(jnp.int32, (16, 128), 1)
    row = lax.broadcasted_iota(jnp.int32, (16, 128), 0)
    spread = (lane % 16 == row).astype(BF)
    chan = lax.broadcasted_iota(jnp.int32, (CB, 128), 0)
    keep = chan % 8 == lax.broadcasted_iota(jnp.int32, (CB, 128), 1) // 16
    out_row = lax.broadcasted_iota(jnp.int32, (128, CB), 0)
    out_chan = lax.broadcasted_iota(jnp.int32, (128, CB), 1)
    packed = None
    for b in range(steps):
        tiled = lax.dot_general(
            small[b].astype(BF), spread, (((0,), (0,)), ((), ())), preferred_element_type=F32
        )
        masked = jnp.where(keep, tiled, 0.0).astype(BF)
        ch = out_chan + b * CB
        take = (out_row // 32 == (ch // 16) % 4) & ((out_row // 2) % 16 == ch // 64) & (out_row % 2 == (ch // 8) % 2)
        part = dot(take.astype(BF), masked)
        packed = part if packed is None else packed + part
    packed = packed.astype(BF)
    for yc in range(4):
        payload[yc, 256:] = packed[yc * 32 : yc * 32 + 32]
    for b in range(steps):
        for copy in out_copies(b):
            copy.wait()


def query_kernel(halo, pm, hspec, up, skip, fxh, fhalo, th, gqmr):
    x, h = dot(fxh[...], pm[...]) + dot(fhalo[...], halo[...]), hspec[...]
    xr, xi, hr, hi = x[:HALF], x[HALF:], h[:HALF], h[HALF:]
    spec = jnp.concatenate([(xr * hr - xi * hi).astype(BF), (xi * hr + xr * hi).astype(BF)], 0)
    ym = dot(th[...], spec)[:ROWS]
    for at in range(0, ROWS, CHUNK):
        s = slice(at, at + CHUNK)
        gqmr[s] = (up[s].astype(F32) * (ym[s] + skip[...] * pm[s].astype(F32))).astype(BF)


def merge_kernel(got, out):
    total = got[0].astype(F32)
    for k in range(1, 4):
        total = total + got[k].astype(F32)
    for z in range(16):
        out[z, :16] = total[z * 16 : z * 16 + 16].astype(BF)
        pair = total[256 + z * 2 : 256 + z * 2 + 2]
        out[z, 16:] = jnp.concatenate([pair, jnp.zeros((6, 128), F32)], 0).astype(BF)


def final_kernel(got, se_o, mr_o, skip_o, gain_o, *, factor):
    total = got[0].astype(F32)
    for k in range(1, 16):
        total = total + got[k].astype(F32)
    total = total * factor
    mr_o[...] = total[:16]
    chan = lax.broadcasted_iota(jnp.int32, (16, 128), 0)
    lane = lax.broadcasted_iota(jnp.int32, (16, 128), 1)
    mine = jnp.where(chan < 8, total[16:17], total[17:18])
    mine = jnp.where(lane // 16 == chan % 8, mine, 0.0)
    pick = (lane % 16 == chan).astype(F32)
    small = lax.dot_general(
        pick, mine, (((1,), (1,)), ((), ())), precision=lax.Precision.HIGHEST, preferred_element_type=F32
    )
    se_o[...] = small[:7]
    skip_o[...] = small[7:8]
    gain_o[...] = small[8:9]


def local(
    query_se, key_se, value_se, query_mr, key_mr, upstream, filter_se, filter_mr, skip_mr, norm_gain
):
    chans = query_se.shape[1]
    steps = chans // CB
    size = lax.axis_size("ctx")
    skip2, gain2 = skip_mr.reshape(1, chans), norm_gain.reshape(1, chans)
    fxh, fxl = halves(basis(0, ROWS))
    fhead, _ = halves(basis(ROWS, ROWS + HEAD))
    fhalo, _ = halves(basis(-HALO, 0))
    back, _ = halves(basis(0, EXT).T * (2.0 / LEN))

    def shape(rows, dtype):
        return jax.ShapeDtypeStruct((rows, chans), dtype)

    def vmem(rows, width, dtype):
        return pltpu.VMEM((rows, width), dtype)

    def kept(x):
        return pltpu.with_memory_space_constraint(x, pltpu.HBM)

    params = pltpu.CompilerParams(vmem_limit_bytes=16 * 1024 * 1024)
    hbm = pl.BlockSpec(memory_space=pltpu.HBM)
    here = pl.BlockSpec(memory_space=pltpu.VMEM)
    fwd, bwd = pl.pallas_call(
        send_kernel,
        in_specs=[hbm] * 6,
        out_shape=[shape(8, BF), shape(BWD, BF)],
        scratch_shapes=[vmem(HEAD, chans, BF)] * 2 + [vmem(8, chans, BF)] * 6 + [pltpu.SemaphoreType.DMA((8,))],
        compiler_params=params,
        name="send",
    )(*(kept(x) for x in (key_se, value_se, query_se, key_mr, upstream, query_mr)))

    down = [(k, k + 1) for k in range(size - 1)]
    upward = [(k + 1, k) for k in range(size - 1)]
    bwd = lax.ppermute(bwd, "ctx", upward)
    fwd = lax.ppermute(fwd, "ctx", down)

    gloc, hspec, conv, mixed, acc = pl.pallas_call(
        local_kernel,
        in_specs=[here] * 6 + [hbm] * 3,
        out_shape=[shape(LEN, F32), shape(LEN, F32), shape(ROWS, F32), shape(ROWS, F32),
                   jax.ShapeDtypeStruct((256, 128), F32)],
        scratch_shapes=[vmem(ROWS + 8, CB, F32), vmem(filter_mr.shape[0], chans, F32), vmem(LEN, ROWS, BF),
                        vmem(LEN, ROWS, BF), pltpu.SemaphoreType.DMA((3,))],
        compiler_params=params,
        name="local",
    )(upstream, query_mr, key_se, value_se, query_se, filter_se, kept(filter_mr), kept(fxh), kept(fxl))

    gp, gext, conv_e, mixed_e, stats = pl.pallas_call(
        norm_kernel,
        out_shape=[shape(EXT, F32), shape(LEN, F32), shape(16, F32), shape(16, F32),
                   jax.ShapeDtypeStruct((8, 8, 128), F32)],
        scratch_shapes=[vmem(32, CB, F32), vmem(256, 128, F32), vmem(256, 128, F32)],
        compiler_params=params,
        name="norm",
    )(fwd, bwd, key_se, value_se, query_se, key_mr, upstream, query_mr, filter_se, gain2, skip2, gloc, hspec,
      mixed, acc, fhead, back)

    stats = lax.all_to_all(stats, "tp", 0, 0, tiled=True)

    gqse, gkse, gvse, gkmr, pm, payload, halo = pl.pallas_call(
        filter_kernel,
        out_specs=[hbm] * 5 + [here] * 2,
        out_shape=[shape(ROWS, BF)] * 5 + [jax.ShapeDtypeStruct((4, 288, 128), BF), shape(HALO, BF)],
        scratch_shapes=[vmem(ROWS + 8, CB, F32), pltpu.VMEM((steps, 16, CB), F32), vmem(256, 128, F32),
                        vmem(256, 128, F32), vmem(EXT, CB, F32)] + [vmem(ROWS, chans, BF)] * 5
        + [pltpu.SemaphoreType.DMA((5, steps))],
        compiler_params=params,
        name="filters",
    )(stats, fwd, bwd, mixed, mixed_e, conv, conv_e, gp, key_mr, query_se, upstream, query_mr, key_se, value_se, gain2,
      filter_se, gext, fxh, back)
    halo = lax.ppermute(halo, "ctx", down)

    def cols(rows):
        return pl.BlockSpec((rows, CB), lambda i: (0, i))

    def whole(*dims):
        return pl.BlockSpec(dims, lambda i: (0,) * len(dims))

    gqmr = pl.pallas_call(
        query_kernel,
        grid=(steps,),
        in_specs=[cols(HALO), cols(ROWS), cols(LEN), cols(ROWS), cols(1), whole(LEN, ROWS), whole(LEN, HALO),
                  whole(EXT, LEN)],
        out_specs=cols(ROWS),
        out_shape=shape(ROWS, BF),
        compiler_params=params,
        name="query",
    )(halo, *(kept(x) for x in (pm, hspec, upstream, skip2, fxh, fhalo, back)))

    near = [[4 * a + b for b in range(4)] for a in range(size // 4)]
    far = [[4 * a + b for a in range(size // 4)] for b in range(4)]
    got = lax.all_to_all(payload, "ctx", 0, 0, axis_index_groups=near, tiled=True)
    merged = pl.pallas_call(
        merge_kernel, out_shape=jax.ShapeDtypeStruct((16, 24, 128), BF), compiler_params=params, name="merge"
    )(got)
    got = lax.all_to_all(merged, "ctx", 0, 0, axis_index_groups=far, tiled=True)
    factor = 1.0 / math.sqrt(ROWS * size)
    se, mr, sk, ga = pl.pallas_call(
        lambda *refs: final_kernel(*refs, factor=factor),
        out_shape=[jax.ShapeDtypeStruct((7, 16), F32), jax.ShapeDtypeStruct((16, 128), F32),
                   jax.ShapeDtypeStruct((1, 16), F32), jax.ShapeDtypeStruct((1, 16), F32)],
        compiler_params=params,
        name="final",
    )(got)
    return (gqse, gkse, gvse, gqmr, gkmr, se, mr.T, sk.reshape(16), ga.reshape(16))


def solution(mesh):
    both, part = P("ctx", "tp"), P(None, "tp")
    in_specs = (both,) * 6 + (part, part, P("tp"), P("tp"))
    split_all = ("tp", "ctx")
    out_specs = (both,) * 5 + (P(None, split_all), P(None, split_all), P(split_all), P(split_all))
    return jax.shard_map(local, mesh=mesh, in_specs=in_specs, out_specs=out_specs, check_vma=False)
```

```python
import math

import jax
import jax.numpy as jnp
import numpy as np
from jax import lax
from jax.experimental import pallas as pl
from jax.experimental.pallas import tpu as pltpu
from jax.sharding import PartitionSpec as P


D = 8192
EPSILON = 0.1
BF = jnp.bfloat16
F32 = jnp.float32

LEN = 384
HALF = LEN // 2
ROWS = 224
EXT = ROWS + 8
HALO = 128
HEAD = 136
CB = 256
BWD = HEAD + 24
CHUNK = 32


def basis(first, last):
    theta = np.pi * (2 * np.arange(HALF)[:, None] + 1) / LEN * np.arange(first, last)[None, :]
    return np.concatenate([np.cos(theta), -np.sin(theta)], 0)


def owner_rows(chans):
    row, chan = np.arange(128)[:, None], np.arange(chans)[None, :]
    near = row // 32 == (chan // 16) % 4
    return near & ((row // 2) % 16 == chan // 64) & (row % 2 == (chan // 8) % 2)


def halves(matrix):
    high = matrix.astype(BF)
    low = (matrix - high.astype(np.float64)).astype(BF)
    return high, low


def dot(a, b):
    return jnp.dot(a, b, preferred_element_type=F32)


def split(x):
    high = x.astype(BF)
    return high, (x - high.astype(F32)).astype(BF)


def forward(fh, fl, data):
    return dot(fh, data) + dot(fl, data)


def wide(column):
    return jnp.concatenate([column] * (CB // 128), axis=1)


def folded(x):
    total = x[:, :128]
    for at in range(128, x.shape[1], 128):
        total = total + x[:, at : at + 128]
    return total


def sums_in_lanes(acc):
    ones = jnp.ones((8, 128), F32)
    return lax.dot_general(
        ones, acc, (((1,), (1,)), ((), ())), precision=lax.Precision.HIGHEST, preferred_element_type=F32
    )


def shifted(ref, row, count):
    return jnp.concatenate([ref[half, pl.ds(row, count), :] for half in range(CB // 128)], 1)


def keep(ref, rows, value):
    for half in range(CB // 128):
        ref[half, rows] = value[:, half * 128 : half * 128 + 128]


def short_conv(ref, taps, row, count):
    total = None
    for step in range(7):
        term = taps[step : step + 1, :] * shifted(ref, row - step, count)
        total = term if total is None else total + term
    return total


def short_adjoint(ref, taps, row, count):
    total = None
    for step in range(7):
        term = taps[step : step + 1, :] * shifted(ref, row + step, count)
        total = term if total is None else total + term
    return total


def rounded(x):
    return x.astype(BF).astype(F32)


def block(b):
    return pl.ds(pl.multiple_of(b * CB, CB), CB)


def eights(x):
    total = x[:8]
    for r in range(8, x.shape[0], 8):
        total = total + x[r : r + 8]
    return total


def send_kernel(
    kse, vse, qse, kmr, up, qmr, fwd, bwd, up_h, qmr_h, kse_h, vse_h, qse_h, kmr_h, kse_t, vse_t, sems
):
    tail = pl.ds(ROWS - 8, 8)
    head = pl.ds(0, 8)
    pieces = [
        (up.at[pl.ds(0, HEAD)], up_h), (qmr.at[pl.ds(0, HEAD)], qmr_h), (qse.at[head], qse_h), (kmr.at[head], kmr_h),
        (kse.at[head], kse_h), (vse.at[head], vse_h), (kse.at[tail], kse_t), (vse.at[tail], vse_t),
    ]
    copies = [pltpu.make_async_copy(src, dst, sems.at[k]) for k, (src, dst) in enumerate(pieces)]
    for copy in copies:
        copy.start()
    for copy in copies:
        copy.wait()

    def step(b, carry):
        c = block(b)
        bwd[:HEAD, c] = (up_h[:, c].astype(F32) * qmr_h[:, c].astype(F32)).astype(BF)
        bwd[HEAD : HEAD + 8, c] = qse_h[:, c]
        bwd[HEAD + 8 : HEAD + 16, c] = kmr_h[:, c]
        bwd[HEAD + 16 :, c] = (kse_h[:, c].astype(F32) * vse_h[:, c].astype(F32)).astype(BF)
        fwd[:, c] = (kse_t[:, c].astype(F32) * vse_t[:, c].astype(F32)).astype(BF)
        return carry

    lax.fori_loop(0, fwd.shape[1] // CB, step, 0)


def local_kernel(
    up, qmr, kse, vse, qse, fse, fmr_in, fxh_in, fxl_in, gloc, hspec, conv_o, mixed_o, acc_o, p_o, g_o,
    prod, fmr, fxh, fxl, sems
):
    pieces = ((fmr_in, fmr), (fxh_in, fxh), (fxl_in, fxl))
    copies = [pltpu.make_async_copy(src, dst, sems.at[k]) for k, (src, dst) in enumerate(pieces)]
    for copy in copies:
        copy.start()
    acc_o[...] = jnp.zeros_like(acc_o)
    prod[:, :8] = jnp.zeros((CB // 128, 8, 128), F32)
    steps = up.shape[1] // CB

    def short(b, carry):
        c = block(b)
        product = rounded(kse[:, c].astype(F32) * vse[:, c].astype(F32))
        keep(prod, slice(8, None), product)
        p_o[:, c] = product
        taps = fse[:, c]
        for at in range(0, ROWS, CHUNK):
            conv = short_conv(prod, taps, 8 + at, CHUNK)
            mixed = qse[at : at + CHUNK, c].astype(F32) * conv
            conv_o[at : at + CHUNK, c] = conv
            mixed_o[at : at + CHUNK, c] = mixed
            square = folded(mixed * mixed)
            if at == 0:
                acc_o[8:CHUNK] += square[8:]
            else:
                acc_o[at : at + CHUNK] += square
        return carry

    lax.fori_loop(0, steps, short, 0)
    for copy in copies:
        copy.wait()

    def spectra(b, carry):
        c = block(b)
        g = (up[:, c].astype(F32) * qmr[:, c].astype(F32)).astype(BF)
        g_o[:, c] = g.astype(F32)
        gloc[:, c] = forward(fxh[...], fxl[...], g)
        high, low = split(fmr[:, c])
        fh = fxh[:, :128]
        hspec[:, c] = dot(fh, high) + dot(fxl[:, :128], high) + dot(fh, low)
        return carry

    lax.fori_loop(0, steps, spectra, 0)


def norm_kernel(
    fwd, bwd, p, g_in, qse, kmr, fse, gain, skip, gloc, hspec, mixed, acc_in, fhh, th,
    gp_o, gext_o, conv_e, mixed_e, stats, prod, acc_sq, acc_w
):
    acc_sq[...] = acc_in[...]
    acc_w[...] = jnp.zeros_like(acc_w)

    def step(b, carry):
        c = block(b)
        spec = gloc[:, c] + dot(fhh[...], bwd[:HEAD, c])
        gext_o[:, c] = spec
        h = hspec[:, c]
        gr, gi, hr, hi = spec[:HALF], spec[HALF:], h[:HALF], h[HALF:]
        back = jnp.concatenate([(gr * hr + gi * hi).astype(BF), (gi * hr - gr * hi).astype(BF)], 0)
        gp_o[:, c] = dot(th[...], back)
        taps, gains, skips = fse[:, c], gain[:, c], skip[:, c]
        keep(prod, slice(0, 8), fwd[:, c].astype(F32))
        keep(prod, slice(8, 16), p[:8, c])
        keep(prod, slice(16, 24), p[ROWS - 8 :, c])
        keep(prod, slice(24, 32), bwd[HEAD + 16 :, c].astype(F32))
        edges = []
        for k, query in ((0, qse[:8, c]), (1, bwd[HEAD : HEAD + 8, c])):
            conv = short_conv(prod, taps, 8 + 16 * k, 8)
            edge = query.astype(F32) * conv
            conv_e[8 * k : 8 * k + 8, c] = conv
            mixed_e[8 * k : 8 * k + 8, c] = edge
            edges.append(edge)
            at = ROWS * k
            acc_sq[at : at + 8] += folded(edge * edge)

        def rows(at, count, mix, key, g):
            gp = gp_o[at : at + count, c] + skips * g
            gp_o[at : at + count, c] = gp
            acc_w[at : at + count] += folded(gp * key.astype(F32) * gains * mix)

        for at in range(0, ROWS, CHUNK):
            s = slice(at, at + CHUNK)
            mix = mixed[s, c]
            if at == 0:
                mix = jnp.concatenate([edges[0], mix[8:]], 0)
            rows(at, CHUNK, mix, kmr[s, c], g_in[s, c])
        rows(ROWS, 8, edges[1], bwd[HEAD + 8 : HEAD + 16, c], bwd[:8, c].astype(F32))
        return carry

    lax.fori_loop(0, gloc.shape[1] // CB, step, 0)
    sq = sums_in_lanes(acc_sq[...])
    w = sums_in_lanes(acc_w[...])
    mine = jnp.concatenate([sq[:1, :128], sq[:1, 128:], w[:1, :128], w[:1, 128:], jnp.zeros((4, 128), F32)], 0)
    for dev in range(8):
        stats[dev] = mine


def column(total, row):
    pick = (lax.broadcasted_iota(jnp.int32, (8, 128), 0) == row).astype(F32)
    return lax.dot_general(
        total, pick, (((0,), (0,)), ((), ())), precision=lax.Precision.HIGHEST, preferred_element_type=F32
    )


def merged_rows(body, edge, at, count, c=slice(None)):
    rows = body[at : at + count, c]
    return jnp.concatenate([edge[:8, c], rows[8:]], 0) if at == 0 else rows


def scales(stats, scale_s, coef_s):
    total = stats[0]
    for dev in range(1, 8):
        total = total + stats[dev]
    s0 = lax.rsqrt(column(total, 0) / D + EPSILON)
    s1 = lax.rsqrt(column(total, 1) / D + EPSILON)
    scale_s[:128] = s0
    scale_s[128:] = s1
    coef_s[:128] = s0 * s0 * s0 * (column(total, 2) / D)
    coef_s[128:] = s1 * s1 * s1 * (column(total, 3) / D)


def filter_kernel(
    stats, fwd, bwd, p, g_in, mixed, mixed_e, conv, conv_e, gp, kmr, qse, kse, vse, gain, fse, gext, fxh, th, spots,
    gqse, gkse, gvse, gkmr, pm_o, payload, halo, prod, small, scale_s, coef_s, gcs, o0, o1, o2, o3, pms, sems
):
    steps = gext.shape[1] // CB
    scales(stats, scale_s, coef_s)
    outs = ((pms, pm_o), (o0, gqse), (o3, gkmr), (o1, gkse), (o2, gvse))

    def out_copies(b):
        c = block(b)
        return [pltpu.make_async_copy(src.at[:, c], dst.at[:, c], sems.at[k, b]) for k, (src, dst) in enumerate(outs)]

    def step(b, carry):
        c = block(b)
        keep(prod, slice(0, 8), fwd[:, c].astype(F32))
        keep(prod, slice(8, None), p[:, c])
        gains = gain[:, c]
        sums = [jnp.zeros((8, CB), F32) for _ in range(9)]
        for at in range(0, ROWS, CHUNK):
            s = slice(at, at + CHUNK)
            mix = merged_rows(mixed, mixed_e, at, CHUNK, c)
            scale = wide(scale_s[s])
            key = kmr[s, c].astype(F32)
            grad = gp[s, c]
            gn = grad * key
            ms = mix * scale
            normed = ms * gains
            pm = (key * normed).astype(BF)
            pms[s, c] = pm
            o3[s, c] = (grad * normed).astype(BF)
            if at >= ROWS - HALO:
                halo[at - (ROWS - HALO) : at - (ROWS - HALO) + CHUNK, c] = pm
            gm = gains * scale * gn - mix * wide(coef_s[s])
            o0[s, c] = (gm * merged_rows(conv, conv_e, at, CHUNK, c)).astype(BF)
            gc = rounded(gm * qse[s, c].astype(F32))
            keep(gcs, s, gc)
            for tap in range(7):
                sums[tap] = sums[tap] + eights(gc * shifted(prod, 8 + at - tap, CHUNK))
            sums[7] = sums[7] + eights(g_in[s, c] * pm.astype(F32))
            sums[8] = sums[8] + eights(gn * ms)
        nxt = slice(ROWS, ROWS + 8)
        gn = gp[nxt, c] * bwd[HEAD + 8 : HEAD + 16, c].astype(F32)
        gm = gains * wide(scale_s[nxt]) * gn - mixed_e[8:, c] * wide(coef_s[nxt])
        keep(gcs, nxt, rounded(gm * bwd[HEAD : HEAD + 8, c].astype(F32)))
        parts = [jnp.sum(x, axis=0, keepdims=True) for x in sums]
        small[b] = jnp.concatenate(parts + [jnp.zeros((7, CB), F32)], 0)

        x = dot(fxh[...], pms[:, c])
        ge = gext[:, c]
        xr, xi, gr, gi = x[:HALF], x[HALF:], ge[:HALF], ge[HALF:]
        back = jnp.concatenate([(gr * xr + gi * xi).astype(BF), (gi * xr - gr * xi).astype(BF)], 0)
        corr = dot(th[:128], back).T.astype(BF)
        for zz in range(4):
            for yc in range(4):
                at = pl.multiple_of((4 * b + zz) * 16, 16)
                payload[yc, pl.ds(at, 16), :] = corr[zz * 64 + yc * 16 : zz * 64 + yc * 16 + 16]
        taps = fse[:, c]
        for at in range(0, ROWS, CHUNK):
            s = slice(at, at + CHUNK)
            gps = short_adjoint(gcs, taps, at, CHUNK)
            o1[s, c] = (gps * vse[s, c].astype(F32)).astype(BF)
            o2[s, c] = (gps * kse[s, c].astype(F32)).astype(BF)
        for copy in out_copies(b):
            copy.start()
        return carry

    lax.fori_loop(0, steps, step, 0)

    lane = lax.broadcasted_iota(jnp.int32, (16, 128), 1)
    row = lax.broadcasted_iota(jnp.int32, (16, 128), 0)
    spread = (lane % 16 == row).astype(BF)
    chan = lax.broadcasted_iota(jnp.int32, (CB, 128), 0)
    own = chan % 8 == lax.broadcasted_iota(jnp.int32, (CB, 128), 1) // 16
    packed = None
    for b in range(steps):
        tiled = lax.dot_general(
            small[b].astype(BF), spread, (((0,), (0,)), ((), ())), preferred_element_type=F32
        )
        masked = jnp.where(own, tiled, 0.0).astype(BF)
        part = dot(spots[:, b * CB : b * CB + CB], masked)
        packed = part if packed is None else packed + part
    packed = packed.astype(BF)
    for yc in range(4):
        payload[yc, 256:] = packed[yc * 32 : yc * 32 + 32]
    for b in range(steps):
        for copy in out_copies(b):
            copy.wait()


def query_kernel(
    halo, pm_in, hspec_in, up_in, skip, fxh_in, fhalo_in, th_in, gqmr,
    pm, hspec, up, fxh, fhalo, th, out, sems, fixed_sems
):
    steps = pm.shape[1] // CB

    def copies(b):
        c = block(b)
        pairs = ((pm_in, pm), (hspec_in, hspec), (up_in, up))
        return [pltpu.make_async_copy(src.at[:, c], dst.at[:, c], sems.at[k, b]) for k, (src, dst) in enumerate(pairs)]

    def out_copy(b):
        c = block(b)
        return pltpu.make_async_copy(out.at[:, c], gqmr.at[:, c], sems.at[3, b])

    bases = [
        pltpu.make_async_copy(src, dst, fixed_sems.at[k])
        for k, (src, dst) in enumerate(((fxh_in, fxh), (fhalo_in, fhalo), (th_in, th)))
    ]
    for copy in bases:
        copy.start()
    for b in range(steps):
        for copy in copies(b):
            copy.start()
    for copy in bases:
        copy.wait()

    def step(b, carry):
        for copy in copies(b):
            copy.wait()
        c = block(b)
        x, h = dot(fxh[...], pm[:, c]) + dot(fhalo[...], halo[:, c]), hspec[:, c]
        xr, xi, hr, hi = x[:HALF], x[HALF:], h[:HALF], h[HALF:]
        spec = jnp.concatenate([(xr * hr - xi * hi).astype(BF), (xi * hr + xr * hi).astype(BF)], 0)
        ym = dot(th[...], spec)
        for at in range(0, ROWS, CHUNK):
            s = slice(at, at + CHUNK)
            out[s, c] = (up[s, c].astype(F32) * (ym[s] + skip[:, c] * pm[s, c].astype(F32))).astype(BF)
        out_copy(b).start()
        return carry

    lax.fori_loop(0, steps, step, 0)
    for b in range(steps):
        out_copy(b).wait()


def merge_kernel(got, out):
    total = got[0].astype(F32)
    for k in range(1, 4):
        total = total + got[k].astype(F32)
    for z in range(16):
        for k in range(9):
            at = z * 16 + 2 * k if k < 8 else 256 + 2 * z
            out[z, :, 128 * k : 128 * k + 128] = total[at : at + 2].astype(BF)


def final_kernel(got, se_o, mr_o, skip_o, gain_o, *, factor):
    packed = got[0].astype(F32)
    for k in range(1, 16):
        packed = packed + got[k].astype(F32)
    total = jnp.concatenate([packed[:, 128 * k : 128 * k + 128] for k in range(9)], 0)
    total = total * factor
    mr_o[...] = total[:16]
    chan = lax.broadcasted_iota(jnp.int32, (16, 128), 0)
    lane = lax.broadcasted_iota(jnp.int32, (16, 128), 1)
    mine = jnp.where(chan < 8, total[16:17], total[17:18])
    mine = jnp.where(lane // 16 == chan % 8, mine, 0.0)
    pick = (lane % 16 == chan).astype(F32)
    small = lax.dot_general(
        pick, mine, (((1,), (1,)), ((), ())), precision=lax.Precision.HIGHEST, preferred_element_type=F32
    )
    se_o[...] = small[:7]
    skip_o[...] = small[7:8]
    gain_o[...] = small[8:9]


def local(
    query_se, key_se, value_se, query_mr, key_mr, upstream, filter_se, filter_mr, skip_mr, norm_gain
):
    chans = query_se.shape[1]
    steps = chans // CB
    size = lax.axis_size("ctx")
    skip2, gain2 = skip_mr.reshape(1, chans), norm_gain.reshape(1, chans)
    fxh, fxl = halves(basis(0, ROWS))
    fhead, _ = halves(basis(ROWS, ROWS + HEAD))
    fhalo, _ = halves(basis(-HALO, 0))
    back, _ = halves(basis(0, EXT).T * (2.0 / LEN))

    def shape(rows, dtype):
        return jax.ShapeDtypeStruct((rows, chans), dtype)

    def vmem(rows, width, dtype):
        return pltpu.VMEM((rows, width), dtype)

    def shifts(rows):
        return pltpu.VMEM((CB // 128, rows, 128), F32)

    def kept(x):
        return pltpu.with_memory_space_constraint(x, pltpu.HBM)

    params = pltpu.CompilerParams(vmem_limit_bytes=16 * 1024 * 1024)
    hbm = pl.BlockSpec(memory_space=pltpu.HBM)
    here = pl.BlockSpec(memory_space=pltpu.VMEM)
    fwd, bwd = pl.pallas_call(
        send_kernel,
        in_specs=[hbm] * 6,
        out_shape=[shape(8, BF), shape(BWD, BF)],
        scratch_shapes=[vmem(HEAD, chans, BF)] * 2 + [vmem(8, chans, BF)] * 6 + [pltpu.SemaphoreType.DMA((8,))],
        compiler_params=params,
        name="send",
    )(*(kept(x) for x in (key_se, value_se, query_se, key_mr, upstream, query_mr)))

    down = [(k, k + 1) for k in range(size - 1)]
    upward = [(k + 1, k) for k in range(size - 1)]
    bwd = lax.ppermute(bwd, "ctx", upward)
    fwd = lax.ppermute(fwd, "ctx", down)

    gloc, hspec, conv, mixed, acc, p, g = pl.pallas_call(
        local_kernel,
        in_specs=[here] * 6 + [hbm] * 3,
        out_shape=[shape(LEN, F32), shape(LEN, F32), shape(ROWS, F32), shape(ROWS, F32),
                   jax.ShapeDtypeStruct((256, 128), F32), shape(ROWS, F32), shape(ROWS, F32)],
        scratch_shapes=[shifts(ROWS + 8), vmem(filter_mr.shape[0], chans, F32), vmem(LEN, ROWS, BF),
                        vmem(LEN, ROWS, BF), pltpu.SemaphoreType.DMA((3,))],
        compiler_params=params,
        name="local",
    )(upstream, query_mr, key_se, value_se, query_se, filter_se, kept(filter_mr), kept(fxh), kept(fxl))

    gp, gext, conv_e, mixed_e, stats = pl.pallas_call(
        norm_kernel,
        out_shape=[shape(EXT, F32), shape(LEN, F32), shape(16, F32), shape(16, F32),
                   jax.ShapeDtypeStruct((8, 8, 128), F32)],
        scratch_shapes=[shifts(32), vmem(256, 128, F32), vmem(256, 128, F32)],
        compiler_params=params,
        name="norm",
    )(fwd, bwd, p, g, query_se, key_mr, filter_se, gain2, skip2, gloc, hspec,
      mixed, acc, fhead, back)

    stats = lax.all_to_all(stats, "tp", 0, 0, tiled=True)

    gqse, gkse, gvse, gkmr, pm, payload, halo = pl.pallas_call(
        filter_kernel,
        out_specs=[hbm] * 5 + [here] * 2,
        out_shape=[shape(ROWS, BF)] * 4
        + [pltpu.HBM((ROWS, chans), BF), jax.ShapeDtypeStruct((4, 288, 128), BF), shape(HALO, BF)],
        scratch_shapes=[shifts(ROWS + 8), pltpu.VMEM((steps, 16, CB), F32), vmem(256, 128, F32),
                        vmem(256, 128, F32), shifts(EXT)] + [vmem(ROWS, chans, BF)] * 5
        + [pltpu.SemaphoreType.DMA((5, steps))],
        compiler_params=params,
        name="filters",
    )(stats, fwd, bwd, p, g, mixed, mixed_e, conv, conv_e, gp, key_mr, query_se, key_se, value_se, gain2, filter_se, gext,
      fxh, back, owner_rows(chans).astype(BF))
    halo = lax.ppermute(halo, "ctx", down)

    gqmr = pl.pallas_call(
        query_kernel,
        in_specs=[here] + [hbm] * 3 + [here] + [hbm] * 3,
        out_specs=hbm,
        out_shape=shape(ROWS, BF),
        scratch_shapes=[vmem(ROWS, chans, BF), vmem(LEN, chans, F32), vmem(ROWS, chans, BF), vmem(LEN, ROWS, BF),
                        vmem(LEN, HALO, BF), vmem(EXT, LEN, BF), vmem(ROWS, chans, BF),
                        pltpu.SemaphoreType.DMA((4, steps)), pltpu.SemaphoreType.DMA((3,))],
        compiler_params=params,
        name="query",
    )(halo, kept(pm), kept(hspec), kept(upstream), skip2, kept(fxh), kept(fhalo), kept(back))

    near = [[4 * a + b for b in range(4)] for a in range(size // 4)]
    far = [[4 * a + b for a in range(size // 4)] for b in range(4)]
    got = lax.all_to_all(payload, "ctx", 0, 0, axis_index_groups=near, tiled=True)
    merged = pl.pallas_call(
        merge_kernel, out_shape=jax.ShapeDtypeStruct((16, 2, 1152), BF), compiler_params=params, name="merge"
    )(got)
    got = lax.all_to_all(merged, "ctx", 0, 0, axis_index_groups=far, tiled=True)
    factor = 1.0 / math.sqrt(ROWS * size)
    se, mr, sk, ga = pl.pallas_call(
        lambda *refs: final_kernel(*refs, factor=factor),
        out_shape=[jax.ShapeDtypeStruct((7, 16), F32), jax.ShapeDtypeStruct((16, 128), F32),
                   jax.ShapeDtypeStruct((1, 16), F32), jax.ShapeDtypeStruct((1, 16), F32)],
        compiler_params=params,
        name="final",
    )(got)
    return (gqse, gkse, gvse, gqmr, gkmr, se, mr.T, sk.reshape(16), ga.reshape(16))


def solution(mesh):
    both, part = P("ctx", "tp"), P(None, "tp")
    in_specs = (both,) * 6 + (part, part, P("tp"), P("tp"))
    split_all = ("tp", "ctx")
    out_specs = (both,) * 5 + (P(None, split_all), P(None, split_all), P(split_all), P(split_all))
    return jax.shard_map(local, mesh=mesh, in_specs=in_specs, out_specs=out_specs, check_vma=False)
```

```python
import math

import jax
import jax.numpy as jnp
import numpy as np
from jax import lax
from jax.experimental import pallas as pl
from jax.experimental.pallas import tpu as pltpu
from jax.sharding import PartitionSpec as P


D = 8192
EPSILON = 0.1
BF = jnp.bfloat16
F32 = jnp.float32

LEN = 384
HALF = LEN // 2
ROWS = 224
EXT = ROWS + 8
HALO = 128
HEAD = 136
CB = 256
BWD = HEAD + 24
CHUNK = 32


def basis(first, last):
    theta = np.pi * (2 * np.arange(HALF)[:, None] + 1) / LEN * np.arange(first, last)[None, :]
    return np.concatenate([np.cos(theta), -np.sin(theta)], 0)


def owner_rows(chans):
    row, chan = np.arange(128)[:, None], np.arange(chans)[None, :]
    near = row // 32 == (chan // 16) % 4
    return near & ((row // 2) % 16 == chan // 64) & (row % 2 == (chan // 8) % 2)


def halves(matrix):
    high = matrix.astype(BF)
    low = (matrix - high.astype(np.float64)).astype(BF)
    return high, low


def dot(a, b):
    return jnp.dot(a, b, preferred_element_type=F32)


def split(x):
    high = x.astype(BF)
    return high, (x - high.astype(F32)).astype(BF)


def forward(fh, fl, data):
    return dot(fh, data) + dot(fl, data)


def wide(column):
    return jnp.concatenate([column] * (CB // 128), axis=1)


def folded(x):
    total = x[:, :128]
    for at in range(128, x.shape[1], 128):
        total = total + x[:, at : at + 128]
    return total


def sums_in_lanes(acc):
    ones = jnp.ones((8, 128), F32)
    return lax.dot_general(
        ones, acc, (((1,), (1,)), ((), ())), precision=lax.Precision.HIGHEST, preferred_element_type=F32
    )


def shifted(ref, row, count):
    return jnp.concatenate([ref[half, pl.ds(row, count), :] for half in range(CB // 128)], 1)


def keep(ref, rows, value):
    for half in range(CB // 128):
        ref[half, rows] = value[:, half * 128 : half * 128 + 128]


def short_conv(ref, taps, row, count):
    total = None
    for step in range(7):
        term = taps[step : step + 1, :] * shifted(ref, row - step, count)
        total = term if total is None else total + term
    return total


def short_adjoint(ref, taps, row, count):
    total = None
    for step in range(7):
        term = taps[step : step + 1, :] * shifted(ref, row + step, count)
        total = term if total is None else total + term
    return total


def rounded(x):
    return x.astype(BF).astype(F32)


def block(b):
    return pl.ds(pl.multiple_of(b * CB, CB), CB)


def eights(x):
    total = x[:8]
    for r in range(8, x.shape[0], 8):
        total = total + x[r : r + 8]
    return total


def send_kernel(
    kse, vse, qse, kmr, up, qmr, fwd, bwd, up_h, qmr_h, kse_h, vse_h, qse_h, kmr_h, kse_t, vse_t, sems
):
    tail = pl.ds(ROWS - 8, 8)
    head = pl.ds(0, 8)
    pieces = [
        (up.at[pl.ds(0, HEAD)], up_h), (qmr.at[pl.ds(0, HEAD)], qmr_h), (qse.at[head], qse_h), (kmr.at[head], kmr_h),
        (kse.at[head], kse_h), (vse.at[head], vse_h), (kse.at[tail], kse_t), (vse.at[tail], vse_t),
    ]
    copies = [pltpu.make_async_copy(src, dst, sems.at[k]) for k, (src, dst) in enumerate(pieces)]
    for copy in copies:
        copy.start()
    for copy in copies:
        copy.wait()

    def step(b, carry):
        c = block(b)
        bwd[:HEAD, c] = (up_h[:, c].astype(F32) * qmr_h[:, c].astype(F32)).astype(BF)
        bwd[HEAD : HEAD + 8, c] = qse_h[:, c]
        bwd[HEAD + 8 : HEAD + 16, c] = kmr_h[:, c]
        bwd[HEAD + 16 :, c] = (kse_h[:, c].astype(F32) * vse_h[:, c].astype(F32)).astype(BF)
        fwd[:, c] = (kse_t[:, c].astype(F32) * vse_t[:, c].astype(F32)).astype(BF)
        return carry

    lax.fori_loop(0, fwd.shape[1] // CB, step, 0)


def local_kernel(
    up, qmr, kse, vse, qse, fse, fmr_in, fxh_in, fxl_in, gloc, hspec, conv_o, mixed_o, acc_o, p_o, g_o,
    prod, fmr, fxh, fxl, sems
):
    pieces = ((fmr_in, fmr), (fxh_in, fxh), (fxl_in, fxl))
    copies = [pltpu.make_async_copy(src, dst, sems.at[k]) for k, (src, dst) in enumerate(pieces)]
    for copy in copies:
        copy.start()
    acc_o[...] = jnp.zeros_like(acc_o)
    prod[:, :8] = jnp.zeros((CB // 128, 8, 128), F32)
    steps = up.shape[1] // CB

    def short(b, carry):
        c = block(b)
        product = rounded(kse[:, c].astype(F32) * vse[:, c].astype(F32))
        keep(prod, slice(8, None), product)
        p_o[:, c] = product
        taps = fse[:, c]
        for at in range(0, ROWS, CHUNK):
            conv = short_conv(prod, taps, 8 + at, CHUNK)
            mixed = qse[at : at + CHUNK, c].astype(F32) * conv
            conv_o[at : at + CHUNK, c] = conv
            mixed_o[at : at + CHUNK, c] = mixed
            square = folded(mixed * mixed)
            if at == 0:
                acc_o[8:CHUNK] += square[8:]
            else:
                acc_o[at : at + CHUNK] += square
        return carry

    lax.fori_loop(0, steps, short, 0)
    for copy in copies:
        copy.wait()

    def spectra(b, carry):
        c = block(b)
        g = (up[:, c].astype(F32) * qmr[:, c].astype(F32)).astype(BF)
        g_o[:, c] = g.astype(F32)
        gloc[:, c] = forward(fxh[...], fxl[...], g)
        high, low = split(fmr[:, c])
        fh = fxh[:, :128]
        hspec[:, c] = dot(fh, high) + dot(fxl[:, :128], high) + dot(fh, low)
        return carry

    lax.fori_loop(0, steps, spectra, 0)


def norm_kernel(
    fwd, bwd, p, g_in, qse, kmr, fse, gain, skip, gloc, hspec, mixed, acc_in, fhh, th,
    gp_o, gext_o, conv_e, mixed_e, stats, prod, acc_sq, acc_w
):
    acc_sq[...] = acc_in[...]
    acc_w[...] = jnp.zeros_like(acc_w)

    def step(b, carry):
        c = block(b)
        spec = gloc[:, c] + dot(fhh[...], bwd[:HEAD, c])
        gext_o[:, c] = spec
        h = hspec[:, c]
        gr, gi, hr, hi = spec[:HALF], spec[HALF:], h[:HALF], h[HALF:]
        back = jnp.concatenate([(gr * hr + gi * hi).astype(BF), (gi * hr - gr * hi).astype(BF)], 0)
        gp_o[:, c] = dot(th[...], back)
        taps, gains, skips = fse[:, c], gain[:, c], skip[:, c]
        keep(prod, slice(0, 8), fwd[:, c].astype(F32))
        keep(prod, slice(8, 16), p[:8, c])
        keep(prod, slice(16, 24), p[ROWS - 8 :, c])
        keep(prod, slice(24, 32), bwd[HEAD + 16 :, c].astype(F32))
        edges = []
        for k, query in ((0, qse[:8, c]), (1, bwd[HEAD : HEAD + 8, c])):
            conv = short_conv(prod, taps, 8 + 16 * k, 8)
            edge = query.astype(F32) * conv
            conv_e[8 * k : 8 * k + 8, c] = conv
            mixed_e[8 * k : 8 * k + 8, c] = edge
            edges.append(edge)
            at = ROWS * k
            acc_sq[at : at + 8] += folded(edge * edge)

        def rows(at, count, mix, key, g):
            gp = gp_o[at : at + count, c] + skips * g
            gp_o[at : at + count, c] = gp
            acc_w[at : at + count] += folded(gp * key.astype(F32) * gains * mix)

        for at in range(0, ROWS, CHUNK):
            s = slice(at, at + CHUNK)
            mix = mixed[s, c]
            if at == 0:
                mix = jnp.concatenate([edges[0], mix[8:]], 0)
            rows(at, CHUNK, mix, kmr[s, c], g_in[s, c])
        rows(ROWS, 8, edges[1], bwd[HEAD + 8 : HEAD + 16, c], bwd[:8, c].astype(F32))
        return carry

    lax.fori_loop(0, gloc.shape[1] // CB, step, 0)
    sq = sums_in_lanes(acc_sq[...])
    w = sums_in_lanes(acc_w[...])
    mine = jnp.concatenate([sq[:1, :128], sq[:1, 128:], w[:1, :128], w[:1, 128:], jnp.zeros((4, 128), F32)], 0)
    for dev in range(8):
        stats[dev] = mine


def column(total, row):
    pick = (lax.broadcasted_iota(jnp.int32, (8, 128), 0) == row).astype(F32)
    return lax.dot_general(
        total, pick, (((0,), (0,)), ((), ())), precision=lax.Precision.HIGHEST, preferred_element_type=F32
    )


def merged_rows(body, edge, at, count, c=slice(None)):
    rows = body[at : at + count, c]
    return jnp.concatenate([edge[:8, c], rows[8:]], 0) if at == 0 else rows


def scales(stats, scale_s, coef_s):
    total = stats[0]
    for dev in range(1, 8):
        total = total + stats[dev]
    s0 = lax.rsqrt(column(total, 0) / D + EPSILON)
    s1 = lax.rsqrt(column(total, 1) / D + EPSILON)
    scale_s[:128] = s0
    scale_s[128:] = s1
    coef_s[:128] = s0 * s0 * s0 * (column(total, 2) / D)
    coef_s[128:] = s1 * s1 * s1 * (column(total, 3) / D)


def filter_kernel(
    stats, fwd, p, g_in, mixed, mixed_e, gp, kmr, qse, gain, gext, fxh, th, spots,
    payload, halo, prod, small, scale_s, coef_s, pms
):
    steps = gext.shape[1] // CB
    scales(stats, scale_s, coef_s)

    def step(b, carry):
        c = block(b)
        keep(prod, slice(0, 8), fwd[:, c].astype(F32))
        keep(prod, slice(8, None), p[:, c])
        gains = gain[:, c]
        sums = [jnp.zeros((8, CB), F32) for _ in range(9)]
        for at in range(0, ROWS, CHUNK):
            s = slice(at, at + CHUNK)
            mix = merged_rows(mixed, mixed_e, at, CHUNK, c)
            scale = wide(scale_s[s])
            key = kmr[s, c].astype(F32)
            grad = gp[s, c]
            gn = grad * key
            ms = mix * scale
            normed = ms * gains
            pm = (key * normed).astype(BF)
            pms[s] = pm
            if at >= ROWS - HALO:
                halo[at - (ROWS - HALO) : at - (ROWS - HALO) + CHUNK, c] = pm
            gm = gains * scale * gn - mix * wide(coef_s[s])
            gc = rounded(gm * qse[s, c].astype(F32))
            for tap in range(7):
                sums[tap] = sums[tap] + eights(gc * shifted(prod, 8 + at - tap, CHUNK))
            sums[7] = sums[7] + eights(g_in[s, c] * pm.astype(F32))
            sums[8] = sums[8] + eights(gn * ms)
        parts = [jnp.sum(x, axis=0, keepdims=True) for x in sums]
        small[b] = jnp.concatenate(parts + [jnp.zeros((7, CB), F32)], 0)

        x = dot(fxh[...], pms[...])
        ge = gext[:, c]
        xr, xi, gr, gi = x[:HALF], x[HALF:], ge[:HALF], ge[HALF:]
        back = jnp.concatenate([(gr * xr + gi * xi).astype(BF), (gi * xr - gr * xi).astype(BF)], 0)
        corr = dot(th[:128], back).T.astype(BF)
        for zz in range(4):
            for yc in range(4):
                at = pl.multiple_of((4 * b + zz) * 16, 16)
                payload[yc, pl.ds(at, 16), :] = corr[zz * 64 + yc * 16 : zz * 64 + yc * 16 + 16]
        return carry

    lax.fori_loop(0, steps, step, 0)

    lane = lax.broadcasted_iota(jnp.int32, (16, 128), 1)
    row = lax.broadcasted_iota(jnp.int32, (16, 128), 0)
    spread = (lane % 16 == row).astype(BF)
    chan = lax.broadcasted_iota(jnp.int32, (CB, 128), 0)
    own = chan % 8 == lax.broadcasted_iota(jnp.int32, (CB, 128), 1) // 16
    packed = None
    for b in range(steps):
        tiled = lax.dot_general(
            small[b].astype(BF), spread, (((0,), (0,)), ((), ())), preferred_element_type=F32
        )
        masked = jnp.where(own, tiled, 0.0).astype(BF)
        part = dot(spots[:, b * CB : b * CB + CB], masked)
        packed = part if packed is None else packed + part
    packed = packed.astype(BF)
    for yc in range(4):
        payload[yc, 256:] = packed[yc * 32 : yc * 32 + 32]


def rest_kernel(
    stats, halo, hspec, mixed, conv, mixed_e, conv_e, gp, bwd, up, kmr, kse, vse, qse, gain, skip, fse, fxh, fhalo, th,
    gqse, gkse, gvse, gqmr, gkmr, scale_s, coef_s, gcs, pms
):
    @pl.when(pl.program_id(0) == 0)
    def _():
        scales(stats, scale_s, coef_s)

    gains, taps, skips = gain[...], fse[...], skip[...]
    for at in range(0, ROWS, CHUNK):
        s = slice(at, at + CHUNK)
        mix = merged_rows(mixed, mixed_e, at, CHUNK)
        con = merged_rows(conv, conv_e, at, CHUNK)
        scale, key, grad = wide(scale_s[s]), kmr[s].astype(F32), gp[s]
        normed = mix * scale * gains
        pms[s] = (key * normed).astype(BF)
        gkmr[s] = (grad * normed).astype(BF)
        gm = gains * scale * (grad * key) - mix * wide(coef_s[s])
        gqse[s] = (gm * con).astype(BF)
        keep(gcs, s, rounded(gm * qse[s].astype(F32)))
    nxt = slice(ROWS, ROWS + 8)
    gn = gp[nxt] * bwd[HEAD + 8 : HEAD + 16].astype(F32)
    gm = gains * wide(scale_s[nxt]) * gn - mixed_e[8:] * wide(coef_s[nxt])
    keep(gcs, nxt, rounded(gm * bwd[HEAD : HEAD + 8].astype(F32)))
    x, h = dot(fxh[...], pms[...]) + dot(fhalo[...], halo[...]), hspec[...]
    xr, xi, hr, hi = x[:HALF], x[HALF:], h[:HALF], h[HALF:]
    spec = jnp.concatenate([(xr * hr - xi * hi).astype(BF), (xi * hr + xr * hi).astype(BF)], 0)
    ym = dot(th[:ROWS], spec)
    for at in range(0, ROWS, CHUNK):
        s = slice(at, at + CHUNK)
        gqmr[s] = (up[s].astype(F32) * (ym[s] + skips * pms[s].astype(F32))).astype(BF)
        gps = short_adjoint(gcs, taps, at, CHUNK)
        gkse[s] = (gps * vse[s].astype(F32)).astype(BF)
        gvse[s] = (gps * kse[s].astype(F32)).astype(BF)


def merge_kernel(got, out):
    total = got[0].astype(F32)
    for k in range(1, 4):
        total = total + got[k].astype(F32)
    for z in range(16):
        for k in range(9):
            at = z * 16 + 2 * k if k < 8 else 256 + 2 * z
            out[z, :, 128 * k : 128 * k + 128] = total[at : at + 2].astype(BF)


def final_kernel(got, se_o, mr_o, skip_o, gain_o, *, factor):
    packed = got[0].astype(F32)
    for k in range(1, 16):
        packed = packed + got[k].astype(F32)
    total = jnp.concatenate([packed[:, 128 * k : 128 * k + 128] for k in range(9)], 0)
    total = total * factor
    mr_o[...] = total[:16]
    chan = lax.broadcasted_iota(jnp.int32, (16, 128), 0)
    lane = lax.broadcasted_iota(jnp.int32, (16, 128), 1)
    mine = jnp.where(chan < 8, total[16:17], total[17:18])
    mine = jnp.where(lane // 16 == chan % 8, mine, 0.0)
    pick = (lane % 16 == chan).astype(F32)
    small = lax.dot_general(
        pick, mine, (((1,), (1,)), ((), ())), precision=lax.Precision.HIGHEST, preferred_element_type=F32
    )
    se_o[...] = small[:7]
    skip_o[...] = small[7:8]
    gain_o[...] = small[8:9]


def local(
    query_se, key_se, value_se, query_mr, key_mr, upstream, filter_se, filter_mr, skip_mr, norm_gain
):
    chans = query_se.shape[1]
    steps = chans // CB
    size = lax.axis_size("ctx")
    skip2, gain2 = skip_mr.reshape(1, chans), norm_gain.reshape(1, chans)
    fxh, fxl = halves(basis(0, ROWS))
    fhead, _ = halves(basis(ROWS, ROWS + HEAD))
    fhalo, _ = halves(basis(-HALO, 0))
    back, _ = halves(basis(0, EXT).T * (2.0 / LEN))

    def shape(rows, dtype):
        return jax.ShapeDtypeStruct((rows, chans), dtype)

    def vmem(rows, width, dtype):
        return pltpu.VMEM((rows, width), dtype)

    def shifts(rows):
        return pltpu.VMEM((CB // 128, rows, 128), F32)

    def kept(x):
        return pltpu.with_memory_space_constraint(x, pltpu.HBM)

    params = pltpu.CompilerParams(vmem_limit_bytes=16 * 1024 * 1024)
    hbm = pl.BlockSpec(memory_space=pltpu.HBM)
    here = pl.BlockSpec(memory_space=pltpu.VMEM)
    fwd, bwd = pl.pallas_call(
        send_kernel,
        in_specs=[hbm] * 6,
        out_shape=[shape(8, BF), shape(BWD, BF)],
        scratch_shapes=[vmem(HEAD, chans, BF)] * 2 + [vmem(8, chans, BF)] * 6 + [pltpu.SemaphoreType.DMA((8,))],
        compiler_params=params,
        name="send",
    )(*(kept(x) for x in (key_se, value_se, query_se, key_mr, upstream, query_mr)))

    down = [(k, k + 1) for k in range(size - 1)]
    upward = [(k + 1, k) for k in range(size - 1)]
    bwd = lax.ppermute(bwd, "ctx", upward)
    fwd = lax.ppermute(fwd, "ctx", down)

    gloc, hspec, conv, mixed, acc, p, g = pl.pallas_call(
        local_kernel,
        in_specs=[here] * 6 + [hbm] * 3,
        out_shape=[shape(LEN, F32), shape(LEN, F32), shape(ROWS, F32), shape(ROWS, F32),
                   jax.ShapeDtypeStruct((256, 128), F32), shape(ROWS, F32), shape(ROWS, F32)],
        scratch_shapes=[shifts(ROWS + 8), vmem(filter_mr.shape[0], chans, F32), vmem(LEN, ROWS, BF),
                        vmem(LEN, ROWS, BF), pltpu.SemaphoreType.DMA((3,))],
        compiler_params=params,
        name="local",
    )(upstream, query_mr, key_se, value_se, query_se, filter_se, kept(filter_mr), kept(fxh), kept(fxl))

    gp, gext, conv_e, mixed_e, stats = pl.pallas_call(
        norm_kernel,
        out_shape=[shape(EXT, F32), shape(LEN, F32), shape(16, F32), shape(16, F32),
                   jax.ShapeDtypeStruct((8, 8, 128), F32)],
        scratch_shapes=[shifts(32), vmem(256, 128, F32), vmem(256, 128, F32)],
        compiler_params=params,
        name="norm",
    )(fwd, bwd, p, g, query_se, key_mr, filter_se, gain2, skip2, gloc, hspec,
      mixed, acc, fhead, back)

    stats = lax.all_to_all(stats, "tp", 0, 0, tiled=True)

    payload, halo = pl.pallas_call(
        filter_kernel,
        out_shape=[jax.ShapeDtypeStruct((4, 288, 128), BF), shape(HALO, BF)],
        scratch_shapes=[shifts(ROWS + 8), pltpu.VMEM((steps, 16, CB), F32), vmem(256, 128, F32), vmem(256, 128, F32),
                        vmem(ROWS, CB, BF)],
        compiler_params=params,
        name="filters",
    )(stats, fwd, p, g, mixed, mixed_e, gp, key_mr, query_se, gain2, gext, fxh, back, owner_rows(chans).astype(BF))
    halo = lax.ppermute(halo, "ctx", down)

    def cols(rows):
        return pl.BlockSpec((rows, CB), lambda i: (0, i))

    def whole(*dims):
        return pl.BlockSpec(dims, lambda i: (0,) * len(dims))

    late = (hspec, mixed, conv, mixed_e, conv_e, gp, bwd, upstream, key_mr, key_se, value_se, query_se, gain2, skip2,
            filter_se)
    bases = (fxh, fhalo, back)
    gqse, gkse, gvse, gqmr, gkmr = pl.pallas_call(
        rest_kernel,
        grid=(steps,),
        in_specs=[whole(8, 8, 128), cols(HALO)] + [cols(x.shape[0]) for x in late] + [whole(*x.shape) for x in bases],
        out_specs=[cols(ROWS)] * 5,
        out_shape=[shape(ROWS, BF)] * 5,
        scratch_shapes=[vmem(256, 128, F32), vmem(256, 128, F32), shifts(EXT), vmem(ROWS, CB, BF)],
        compiler_params=params,
        name="rest",
    )(kept(stats), halo, *(kept(x) for x in late + bases))

    near = [[4 * a + b for b in range(4)] for a in range(size // 4)]
    far = [[4 * a + b for a in range(size // 4)] for b in range(4)]
    got = lax.all_to_all(payload, "ctx", 0, 0, axis_index_groups=near, tiled=True)
    merged = pl.pallas_call(
        merge_kernel, out_shape=jax.ShapeDtypeStruct((16, 2, 1152), BF), compiler_params=params, name="merge"
    )(got)
    got = lax.all_to_all(merged, "ctx", 0, 0, axis_index_groups=far, tiled=True)
    factor = 1.0 / math.sqrt(ROWS * size)
    se, mr, sk, ga = pl.pallas_call(
        lambda *refs: final_kernel(*refs, factor=factor),
        out_shape=[jax.ShapeDtypeStruct((7, 16), F32), jax.ShapeDtypeStruct((16, 128), F32),
                   jax.ShapeDtypeStruct((1, 16), F32), jax.ShapeDtypeStruct((1, 16), F32)],
        compiler_params=params,
        name="final",
    )(got)
    return (gqse, gkse, gvse, gqmr, gkmr, se, mr.T, sk.reshape(16), ga.reshape(16))


def solution(mesh):
    both, part = P("ctx", "tp"), P(None, "tp")
    in_specs = (both,) * 6 + (part, part, P("tp"), P("tp"))
    split_all = ("tp", "ctx")
    out_specs = (both,) * 5 + (P(None, split_all), P(None, split_all), P(split_all), P(split_all))
    return jax.shard_map(local, mesh=mesh, in_specs=in_specs, out_specs=out_specs, check_vma=False)
```

```python
import math

import jax
import jax.numpy as jnp
import numpy as np
from jax import lax
from jax.experimental import pallas as pl
from jax.experimental.pallas import tpu as pltpu
from jax.sharding import PartitionSpec as P


D = 8192
EPSILON = 0.1
BF = jnp.bfloat16
F32 = jnp.float32

LEN = 384
HALF = LEN // 2
ROWS = 224
EXT = ROWS + 8
HALO = 128
HEAD = 136
CB = 256
BWD = HEAD + 24
CHUNK = 32


def basis(first, last):
    theta = np.pi * (2 * np.arange(HALF)[:, None] + 1) / LEN * np.arange(first, last)[None, :]
    return np.concatenate([np.cos(theta), -np.sin(theta)], 0)


def owner_rows(chans):
    row, chan = np.arange(128)[:, None], np.arange(chans)[None, :]
    near = row // 32 == (chan // 16) % 4
    return near & ((row // 2) % 16 == chan // 64) & (row % 2 == (chan // 8) % 2)


def halves(matrix):
    high = matrix.astype(BF)
    low = (matrix - high.astype(np.float64)).astype(BF)
    return high, low


def dot(a, b):
    return jnp.dot(a, b, preferred_element_type=F32)


def split(x):
    high = x.astype(BF)
    return high, (x - high.astype(F32)).astype(BF)


def forward(fh, fl, data):
    return dot(fh, data) + dot(fl, data)


def wide(column):
    return jnp.concatenate([column] * (CB // 128), axis=1)


def folded(x):
    total = x[:, :128]
    for at in range(128, x.shape[1], 128):
        total = total + x[:, at : at + 128]
    return total


def sums_in_lanes(acc):
    ones = jnp.ones((8, 128), F32)
    return lax.dot_general(
        ones, acc, (((1,), (1,)), ((), ())), precision=lax.Precision.HIGHEST, preferred_element_type=F32
    )


def shifted(ref, row, count):
    return jnp.concatenate([ref[half, pl.ds(row, count), :] for half in range(CB // 128)], 1)


def keep(ref, rows, value):
    for half in range(CB // 128):
        ref[half, rows] = value[:, half * 128 : half * 128 + 128]


def short_conv(ref, taps, row, count):
    total = None
    for step in range(7):
        term = taps[step : step + 1, :] * shifted(ref, row - step, count)
        total = term if total is None else total + term
    return total


def short_adjoint(ref, taps, row, count):
    total = None
    for step in range(7):
        term = taps[step : step + 1, :] * shifted(ref, row + step, count)
        total = term if total is None else total + term
    return total


def rounded(x):
    return x.astype(BF).astype(F32)


def block(b):
    return pl.ds(pl.multiple_of(b * CB, CB), CB)


def eights(x):
    total = x[:8]
    for r in range(8, x.shape[0], 8):
        total = total + x[r : r + 8]
    return total


def send_kernel(
    kse, vse, qse, kmr, up, qmr, fwd, bwd, up_h, qmr_h, kse_h, vse_h, qse_h, kmr_h, kse_t, vse_t, sems
):
    tail = pl.ds(ROWS - 8, 8)
    head = pl.ds(0, 8)
    pieces = [
        (up.at[pl.ds(0, HEAD)], up_h), (qmr.at[pl.ds(0, HEAD)], qmr_h), (qse.at[head], qse_h), (kmr.at[head], kmr_h),
        (kse.at[head], kse_h), (vse.at[head], vse_h), (kse.at[tail], kse_t), (vse.at[tail], vse_t),
    ]
    copies = [pltpu.make_async_copy(src, dst, sems.at[k]) for k, (src, dst) in enumerate(pieces)]
    for copy in copies:
        copy.start()
    for copy in copies:
        copy.wait()

    def step(b, carry):
        c = block(b)
        bwd[:HEAD, c] = (up_h[:, c].astype(F32) * qmr_h[:, c].astype(F32)).astype(BF)
        bwd[HEAD : HEAD + 8, c] = qse_h[:, c]
        bwd[HEAD + 8 : HEAD + 16, c] = kmr_h[:, c]
        bwd[HEAD + 16 :, c] = (kse_h[:, c].astype(F32) * vse_h[:, c].astype(F32)).astype(BF)
        fwd[:, c] = (kse_t[:, c].astype(F32) * vse_t[:, c].astype(F32)).astype(BF)
        return carry

    lax.fori_loop(0, fwd.shape[1] // CB, step, 0)


def local_kernel(
    up, qmr, kse, vse, qse, fse, fmr_in, fxh_in, fxl_in, gloc, hspec, hlate, conv_o, mixed_o, acc_o, p_o, g_o,
    prod, fmr, fxh, fxl, sems
):
    pieces = ((fmr_in, fmr), (fxh_in, fxh), (fxl_in, fxl))
    copies = [pltpu.make_async_copy(src, dst, sems.at[k]) for k, (src, dst) in enumerate(pieces)]
    for copy in copies:
        copy.start()
    acc_o[...] = jnp.zeros_like(acc_o)
    prod[:, :8] = jnp.zeros((CB // 128, 8, 128), F32)
    steps = up.shape[1] // CB

    def short(b, carry):
        c = block(b)
        product = rounded(kse[:, c].astype(F32) * vse[:, c].astype(F32))
        keep(prod, slice(8, None), product)
        p_o[:, c] = product
        taps = fse[:, c]
        for at in range(0, ROWS, CHUNK):
            conv = short_conv(prod, taps, 8 + at, CHUNK)
            mixed = qse[at : at + CHUNK, c].astype(F32) * conv
            conv_o[at : at + CHUNK, c] = conv
            mixed_o[at : at + CHUNK, c] = mixed
            square = folded(mixed * mixed)
            if at == 0:
                acc_o[8:CHUNK] += square[8:]
            else:
                acc_o[at : at + CHUNK] += square
        return carry

    lax.fori_loop(0, steps, short, 0)
    for copy in copies:
        copy.wait()

    def spectra(b, carry):
        c = block(b)
        g = (up[:, c].astype(F32) * qmr[:, c].astype(F32)).astype(BF)
        g_o[:, c] = g.astype(F32)
        gloc[:, c] = forward(fxh[...], fxl[...], g)
        high, low = split(fmr[:, c])
        fh = fxh[:, :128]
        h = dot(fh, high) + dot(fxl[:, :128], high) + dot(fh, low)
        hspec[:, c] = h
        hlate[:, c] = h.astype(BF)
        return carry

    lax.fori_loop(0, steps, spectra, 0)


def norm_kernel(
    fwd, bwd, p, g_in, qse, kmr, fse, gain, skip, gloc, hspec, mixed, acc_in, fhh, th,
    gp_o, gext_o, conv_e, mixed_e, stats, prod, acc_sq, acc_w
):
    acc_sq[...] = acc_in[...]
    acc_w[...] = jnp.zeros_like(acc_w)

    def step(b, carry):
        c = block(b)
        spec = gloc[:, c] + dot(fhh[...], bwd[:HEAD, c])
        gext_o[:, c] = spec
        h = hspec[:, c]
        gr, gi, hr, hi = spec[:HALF], spec[HALF:], h[:HALF], h[HALF:]
        back = jnp.concatenate([(gr * hr + gi * hi).astype(BF), (gi * hr - gr * hi).astype(BF)], 0)
        gp_o[:, c] = dot(th[...], back)
        taps, gains, skips = fse[:, c], gain[:, c], skip[:, c]
        keep(prod, slice(0, 8), fwd[:, c].astype(F32))
        keep(prod, slice(8, 16), p[:8, c])
        keep(prod, slice(16, 24), p[ROWS - 8 :, c])
        keep(prod, slice(24, 32), bwd[HEAD + 16 :, c].astype(F32))
        edges = []
        for k, query in ((0, qse[:8, c]), (1, bwd[HEAD : HEAD + 8, c])):
            conv = short_conv(prod, taps, 8 + 16 * k, 8)
            edge = query.astype(F32) * conv
            conv_e[8 * k : 8 * k + 8, c] = conv
            mixed_e[8 * k : 8 * k + 8, c] = edge
            edges.append(edge)
            at = ROWS * k
            acc_sq[at : at + 8] += folded(edge * edge)

        def rows(at, count, mix, key, g):
            gp = gp_o[at : at + count, c] + skips * g
            gp_o[at : at + count, c] = gp
            acc_w[at : at + count] += folded(gp * key.astype(F32) * gains * mix)

        for at in range(0, ROWS, CHUNK):
            s = slice(at, at + CHUNK)
            mix = mixed[s, c]
            if at == 0:
                mix = jnp.concatenate([edges[0], mix[8:]], 0)
            rows(at, CHUNK, mix, kmr[s, c], g_in[s, c])
        rows(ROWS, 8, edges[1], bwd[HEAD + 8 : HEAD + 16, c], bwd[:8, c].astype(F32))
        return carry

    lax.fori_loop(0, gloc.shape[1] // CB, step, 0)
    sq = sums_in_lanes(acc_sq[...])
    w = sums_in_lanes(acc_w[...])
    mine = jnp.concatenate([sq[:1, :128], sq[:1, 128:], w[:1, :128], w[:1, 128:], jnp.zeros((4, 128), F32)], 0)
    for dev in range(8):
        stats[dev] = mine


def column(total, row):
    pick = (lax.broadcasted_iota(jnp.int32, (8, 128), 0) == row).astype(F32)
    return lax.dot_general(
        total, pick, (((0,), (0,)), ((), ())), precision=lax.Precision.HIGHEST, preferred_element_type=F32
    )


def merged_rows(body, edge, at, count, c=slice(None)):
    rows = body[at : at + count, c]
    return jnp.concatenate([edge[:8, c], rows[8:]], 0) if at == 0 else rows


def scales(stats, scale_s, coef_s):
    total = stats[0]
    for dev in range(1, 8):
        total = total + stats[dev]
    s0 = lax.rsqrt(column(total, 0) / D + EPSILON)
    s1 = lax.rsqrt(column(total, 1) / D + EPSILON)
    scale_s[:128] = s0
    scale_s[128:] = s1
    coef_s[:128] = s0 * s0 * s0 * (column(total, 2) / D)
    coef_s[128:] = s1 * s1 * s1 * (column(total, 3) / D)


def filter_kernel(
    stats, fwd, p, g_in, mixed, mixed_e, gp, kmr, qse, gain, gext, fxh, th, spots,
    payload, halo, prod, small, scale_s, coef_s, pms
):
    steps = gext.shape[1] // CB
    scales(stats, scale_s, coef_s)

    def step(b, carry):
        c = block(b)
        keep(prod, slice(0, 8), fwd[:, c].astype(F32))
        keep(prod, slice(8, None), p[:, c])
        gains = gain[:, c]
        sums = [jnp.zeros((8, CB), F32) for _ in range(9)]
        for at in range(0, ROWS, CHUNK):
            s = slice(at, at + CHUNK)
            mix = merged_rows(mixed, mixed_e, at, CHUNK, c)
            scale = wide(scale_s[s])
            key = kmr[s, c].astype(F32)
            grad = gp[s, c]
            gn = grad * key
            ms = mix * scale
            normed = ms * gains
            pm = (key * normed).astype(BF)
            pms[s] = pm
            if at >= ROWS - HALO:
                halo[at - (ROWS - HALO) : at - (ROWS - HALO) + CHUNK, c] = pm
            gm = gains * scale * gn - mix * wide(coef_s[s])
            gc = rounded(gm * qse[s, c].astype(F32))
            for tap in range(7):
                sums[tap] = sums[tap] + eights(gc * shifted(prod, 8 + at - tap, CHUNK))
            sums[7] = sums[7] + eights(g_in[s, c] * pm.astype(F32))
            sums[8] = sums[8] + eights(gn * ms)
        parts = [jnp.sum(x, axis=0, keepdims=True) for x in sums]
        small[b] = jnp.concatenate(parts + [jnp.zeros((7, CB), F32)], 0)

        x = dot(fxh[...], pms[...])
        ge = gext[:, c]
        xr, xi, gr, gi = x[:HALF], x[HALF:], ge[:HALF], ge[HALF:]
        back = jnp.concatenate([(gr * xr + gi * xi).astype(BF), (gi * xr - gr * xi).astype(BF)], 0)
        corr = dot(th[:128], back).T.astype(BF)
        for zz in range(4):
            for yc in range(4):
                at = pl.multiple_of((4 * b + zz) * 16, 16)
                payload[yc, pl.ds(at, 16), :] = corr[zz * 64 + yc * 16 : zz * 64 + yc * 16 + 16]
        return carry

    lax.fori_loop(0, steps, step, 0)

    lane = lax.broadcasted_iota(jnp.int32, (16, 128), 1)
    row = lax.broadcasted_iota(jnp.int32, (16, 128), 0)
    spread = (lane % 16 == row).astype(BF)
    chan = lax.broadcasted_iota(jnp.int32, (CB, 128), 0)
    own = chan % 8 == lax.broadcasted_iota(jnp.int32, (CB, 128), 1) // 16
    packed = None
    for b in range(steps):
        tiled = lax.dot_general(
            small[b].astype(BF), spread, (((0,), (0,)), ((), ())), preferred_element_type=F32
        )
        masked = jnp.where(own, tiled, 0.0).astype(BF)
        part = dot(spots[:, b * CB : b * CB + CB], masked)
        packed = part if packed is None else packed + part
    packed = packed.astype(BF)
    for yc in range(4):
        payload[yc, 256:] = packed[yc * 32 : yc * 32 + 32]


def rest_kernel(
    stats, mixed, conv, mixed_e, conv_e, gp, bwd, kmr, kse, vse, qse, gain, fse,
    gqse, gkse, gvse, gkmr, pm_o, scale_s, coef_s, gcs
):
    @pl.when(pl.program_id(0) == 0)
    def _():
        scales(stats, scale_s, coef_s)

    gains, taps = gain[...], fse[...]
    for at in range(0, ROWS, CHUNK):
        s = slice(at, at + CHUNK)
        mix = merged_rows(mixed, mixed_e, at, CHUNK)
        con = merged_rows(conv, conv_e, at, CHUNK)
        scale, key, grad = wide(scale_s[s]), kmr[s].astype(F32), gp[s]
        normed = mix * scale * gains
        pm_o[s] = (key * normed).astype(BF)
        gkmr[s] = (grad * normed).astype(BF)
        gm = gains * scale * (grad * key) - mix * wide(coef_s[s])
        gqse[s] = (gm * con).astype(BF)
        keep(gcs, s, rounded(gm * qse[s].astype(F32)))
    nxt = slice(ROWS, ROWS + 8)
    gn = gp[nxt] * bwd[HEAD + 8 : HEAD + 16].astype(F32)
    gm = gains * wide(scale_s[nxt]) * gn - mixed_e[8:] * wide(coef_s[nxt])
    keep(gcs, nxt, rounded(gm * bwd[HEAD : HEAD + 8].astype(F32)))
    for at in range(0, ROWS, CHUNK):
        s = slice(at, at + CHUNK)
        gps = short_adjoint(gcs, taps, at, CHUNK)
        gkse[s] = (gps * vse[s].astype(F32)).astype(BF)
        gvse[s] = (gps * kse[s].astype(F32)).astype(BF)


def query_kernel(
    halo, pm_in, hspec_in, up_in, skip, fxh_in, fhalo_in, th_in, gqmr,
    pm, hspec, up, fxh, fhalo, th, out, sems, fixed_sems
):
    steps = pm.shape[1] // CB

    def copies(b):
        c = block(b)
        pairs = ((pm_in, pm), (hspec_in, hspec), (up_in, up))
        return [pltpu.make_async_copy(src.at[:, c], dst.at[:, c], sems.at[k, b]) for k, (src, dst) in enumerate(pairs)]

    def out_copy(b):
        c = block(b)
        return pltpu.make_async_copy(out.at[:, c], gqmr.at[:, c], sems.at[3, b])

    bases = [
        pltpu.make_async_copy(src, dst, fixed_sems.at[k])
        for k, (src, dst) in enumerate(((fxh_in, fxh), (fhalo_in, fhalo), (th_in, th)))
    ]
    for copy in bases:
        copy.start()
    for b in range(steps):
        for copy in copies(b):
            copy.start()
    for copy in bases:
        copy.wait()

    def step(b, carry):
        for copy in copies(b):
            copy.wait()
        c = block(b)
        x, h = dot(fxh[...], pm[:, c]) + dot(fhalo[...], halo[:, c]), hspec[:, c].astype(F32)
        xr, xi, hr, hi = x[:HALF], x[HALF:], h[:HALF], h[HALF:]
        spec = jnp.concatenate([(xr * hr - xi * hi).astype(BF), (xi * hr + xr * hi).astype(BF)], 0)
        ym = dot(th[...], spec)
        for at in range(0, ROWS, CHUNK):
            s = slice(at, at + CHUNK)
            out[s, c] = (up[s, c].astype(F32) * (ym[s] + skip[:, c] * pm[s, c].astype(F32))).astype(BF)
        out_copy(b).start()
        return carry

    lax.fori_loop(0, steps, step, 0)
    for b in range(steps):
        out_copy(b).wait()


def merge_kernel(got, out):
    total = got[0].astype(F32)
    for k in range(1, 4):
        total = total + got[k].astype(F32)
    for z in range(16):
        for k in range(9):
            at = z * 16 + 2 * k if k < 8 else 256 + 2 * z
            out[z, :, 128 * k : 128 * k + 128] = total[at : at + 2].astype(BF)


def final_kernel(got, se_o, mr_o, skip_o, gain_o, *, factor):
    packed = got[0].astype(F32)
    for k in range(1, 16):
        packed = packed + got[k].astype(F32)
    total = jnp.concatenate([packed[:, 128 * k : 128 * k + 128] for k in range(9)], 0)
    total = total * factor
    mr_o[...] = total[:16]
    chan = lax.broadcasted_iota(jnp.int32, (16, 128), 0)
    lane = lax.broadcasted_iota(jnp.int32, (16, 128), 1)
    mine = jnp.where(chan < 8, total[16:17], total[17:18])
    mine = jnp.where(lane // 16 == chan % 8, mine, 0.0)
    pick = (lane % 16 == chan).astype(F32)
    small = lax.dot_general(
        pick, mine, (((1,), (1,)), ((), ())), precision=lax.Precision.HIGHEST, preferred_element_type=F32
    )
    se_o[...] = small[:7]
    skip_o[...] = small[7:8]
    gain_o[...] = small[8:9]


def local(
    query_se, key_se, value_se, query_mr, key_mr, upstream, filter_se, filter_mr, skip_mr, norm_gain
):
    chans = query_se.shape[1]
    steps = chans // CB
    size = lax.axis_size("ctx")
    skip2, gain2 = skip_mr.reshape(1, chans), norm_gain.reshape(1, chans)
    fxh, fxl = halves(basis(0, ROWS))
    fhead, _ = halves(basis(ROWS, ROWS + HEAD))
    fhalo, _ = halves(basis(-HALO, 0))
    back, _ = halves(basis(0, EXT).T * (2.0 / LEN))

    def shape(rows, dtype):
        return jax.ShapeDtypeStruct((rows, chans), dtype)

    def vmem(rows, width, dtype):
        return pltpu.VMEM((rows, width), dtype)

    def shifts(rows):
        return pltpu.VMEM((CB // 128, rows, 128), F32)

    def kept(x):
        return pltpu.with_memory_space_constraint(x, pltpu.HBM)

    params = pltpu.CompilerParams(vmem_limit_bytes=16 * 1024 * 1024)
    hbm = pl.BlockSpec(memory_space=pltpu.HBM)
    here = pl.BlockSpec(memory_space=pltpu.VMEM)
    fwd, bwd = pl.pallas_call(
        send_kernel,
        in_specs=[hbm] * 6,
        out_shape=[shape(8, BF), shape(BWD, BF)],
        scratch_shapes=[vmem(HEAD, chans, BF)] * 2 + [vmem(8, chans, BF)] * 6 + [pltpu.SemaphoreType.DMA((8,))],
        compiler_params=params,
        name="send",
    )(*(kept(x) for x in (key_se, value_se, query_se, key_mr, upstream, query_mr)))

    down = [(k, k + 1) for k in range(size - 1)]
    upward = [(k + 1, k) for k in range(size - 1)]
    bwd = lax.ppermute(bwd, "ctx", upward)
    fwd = lax.ppermute(fwd, "ctx", down)

    gloc, hspec, hlate, conv, mixed, acc, p, g = pl.pallas_call(
        local_kernel,
        in_specs=[here] * 6 + [hbm] * 3,
        out_shape=[shape(LEN, F32), shape(LEN, F32), shape(LEN, BF), shape(ROWS, F32), shape(ROWS, F32),
                   jax.ShapeDtypeStruct((256, 128), F32), shape(ROWS, F32), shape(ROWS, F32)],
        scratch_shapes=[shifts(ROWS + 8), vmem(filter_mr.shape[0], chans, F32), vmem(LEN, ROWS, BF),
                        vmem(LEN, ROWS, BF), pltpu.SemaphoreType.DMA((3,))],
        compiler_params=params,
        name="local",
    )(upstream, query_mr, key_se, value_se, query_se, filter_se, kept(filter_mr), kept(fxh), kept(fxl))

    gp, gext, conv_e, mixed_e, stats = pl.pallas_call(
        norm_kernel,
        out_shape=[shape(EXT, F32), shape(LEN, F32), shape(16, F32), shape(16, F32),
                   jax.ShapeDtypeStruct((8, 8, 128), F32)],
        scratch_shapes=[shifts(32), vmem(256, 128, F32), vmem(256, 128, F32)],
        compiler_params=params,
        name="norm",
    )(fwd, bwd, p, g, query_se, key_mr, filter_se, gain2, skip2, gloc, hspec,
      mixed, acc, fhead, back)

    stats = lax.all_to_all(stats, "tp", 0, 0, tiled=True)

    payload, halo = pl.pallas_call(
        filter_kernel,
        out_shape=[jax.ShapeDtypeStruct((4, 288, 128), BF), shape(HALO, BF)],
        scratch_shapes=[shifts(ROWS + 8), pltpu.VMEM((steps, 16, CB), F32), vmem(256, 128, F32), vmem(256, 128, F32),
                        vmem(ROWS, CB, BF)],
        compiler_params=params,
        name="filters",
    )(stats, fwd, p, g, mixed, mixed_e, gp, key_mr, query_se, gain2, gext, fxh, back, owner_rows(chans).astype(BF))
    halo = lax.ppermute(halo, "ctx", down)

    def cols(rows):
        return pl.BlockSpec((rows, CB), lambda i: (0, i))

    def whole(*dims):
        return pl.BlockSpec(dims, lambda i: (0,) * len(dims))

    late = (mixed, conv, mixed_e, conv_e, gp, bwd, key_mr, key_se, value_se, query_se, gain2, filter_se)
    gqse, gkse, gvse, gkmr, pm = pl.pallas_call(
        rest_kernel,
        grid=(steps,),
        in_specs=[whole(8, 8, 128)] + [cols(x.shape[0]) for x in late],
        out_specs=[cols(ROWS)] * 5,
        out_shape=[shape(ROWS, BF)] * 4 + [pltpu.HBM((ROWS, chans), BF)],
        scratch_shapes=[vmem(256, 128, F32), vmem(256, 128, F32), shifts(EXT)],
        compiler_params=params,
        name="rest",
    )(kept(stats), *(kept(x) for x in late))
    gqmr = pl.pallas_call(
        query_kernel,
        in_specs=[here] + [hbm] * 3 + [here] + [hbm] * 3,
        out_specs=hbm,
        out_shape=shape(ROWS, BF),
        scratch_shapes=[vmem(ROWS, chans, BF), vmem(LEN, chans, BF), vmem(ROWS, chans, BF), vmem(LEN, ROWS, BF),
                        vmem(LEN, HALO, BF), vmem(EXT, LEN, BF), vmem(ROWS, chans, BF),
                        pltpu.SemaphoreType.DMA((4, steps)), pltpu.SemaphoreType.DMA((3,))],
        compiler_params=params,
        name="query",
    )(halo, kept(pm), kept(hlate), kept(upstream), skip2, kept(fxh), kept(fhalo), kept(back))

    near = [[4 * a + b for b in range(4)] for a in range(size // 4)]
    far = [[4 * a + b for a in range(size // 4)] for b in range(4)]
    got = lax.all_to_all(payload, "ctx", 0, 0, axis_index_groups=near, tiled=True)
    merged = pl.pallas_call(
        merge_kernel, out_shape=jax.ShapeDtypeStruct((16, 2, 1152), BF), compiler_params=params, name="merge"
    )(got)
    got = lax.all_to_all(merged, "ctx", 0, 0, axis_index_groups=far, tiled=True)
    factor = 1.0 / math.sqrt(ROWS * size)
    se, mr, sk, ga = pl.pallas_call(
        lambda *refs: final_kernel(*refs, factor=factor),
        out_shape=[jax.ShapeDtypeStruct((7, 16), F32), jax.ShapeDtypeStruct((16, 128), F32),
                   jax.ShapeDtypeStruct((1, 16), F32), jax.ShapeDtypeStruct((1, 16), F32)],
        compiler_params=params,
        name="final",
    )(got)
    return (gqse, gkse, gvse, gqmr, gkmr, se, mr.T, sk.reshape(16), ga.reshape(16))


def solution(mesh):
    both, part = P("ctx", "tp"), P(None, "tp")
    in_specs = (both,) * 6 + (part, part, P("tp"), P("tp"))
    split_all = ("tp", "ctx")
    out_specs = (both,) * 5 + (P(None, split_all), P(None, split_all), P(split_all), P(split_all))
    return jax.shard_map(local, mesh=mesh, in_specs=in_specs, out_specs=out_specs, check_vma=False)
```

```python
import math

import jax
import jax.numpy as jnp
import numpy as np
from jax import lax
from jax.experimental import pallas as pl
from jax.experimental.pallas import tpu as pltpu
from jax.sharding import PartitionSpec as P


D = 8192
EPSILON = 0.1
BF = jnp.bfloat16
F32 = jnp.float32

LEN = 384
HALF = LEN // 2
ROWS = 224
EXT = ROWS + 8
HALO = 128
HEAD = 136
CB = 256
BWD = HEAD + 24
CHUNK = 32


def basis(first, last):
    theta = np.pi * (2 * np.arange(HALF)[:, None] + 1) / LEN * np.arange(first, last)[None, :]
    return np.concatenate([np.cos(theta), -np.sin(theta)], 0)


def owner_rows(chans):
    row, chan = np.arange(128)[:, None], np.arange(chans)[None, :]
    near = row // 32 == (chan // 16) % 4
    return near & ((row // 2) % 16 == chan // 64) & (row % 2 == (chan // 8) % 2)


def halves(matrix):
    high = matrix.astype(BF)
    low = (matrix - high.astype(np.float64)).astype(BF)
    return high, low


def dot(a, b):
    return jnp.dot(a, b, preferred_element_type=F32)


def split(x):
    high = x.astype(BF)
    return high, (x - high.astype(F32)).astype(BF)


def forward(fh, fl, data):
    return dot(fh, data) + dot(fl, data)


def wide(column):
    return jnp.concatenate([column] * (CB // 128), axis=1)


def folded(x):
    total = x[:, :128]
    for at in range(128, x.shape[1], 128):
        total = total + x[:, at : at + 128]
    return total


def sums_in_lanes(acc):
    ones = jnp.ones((8, 128), F32)
    return lax.dot_general(
        ones, acc, (((1,), (1,)), ((), ())), precision=lax.Precision.HIGHEST, preferred_element_type=F32
    )


def shifted(ref, row, count):
    return jnp.concatenate([ref[half, pl.ds(row, count), :] for half in range(CB // 128)], 1)


def keep(ref, rows, value):
    for half in range(CB // 128):
        ref[half, rows] = value[:, half * 128 : half * 128 + 128]


def short_conv(ref, taps, row, count):
    total = None
    for step in range(7):
        term = taps[step : step + 1, :] * shifted(ref, row - step, count)
        total = term if total is None else total + term
    return total


def short_adjoint(ref, taps, row, count):
    total = None
    for step in range(7):
        term = taps[step : step + 1, :] * shifted(ref, row + step, count)
        total = term if total is None else total + term
    return total


def rounded(x):
    return x.astype(BF).astype(F32)


def block(b):
    return pl.ds(pl.multiple_of(b * CB, CB), CB)


def eights(x):
    total = x[:8]
    for r in range(8, x.shape[0], 8):
        total = total + x[r : r + 8]
    return total


def send_kernel(
    kse, vse, qse, kmr, up, qmr, fwd, bwd, up_h, qmr_h, kse_h, vse_h, qse_h, kmr_h, kse_t, vse_t, sems
):
    tail = pl.ds(ROWS - 8, 8)
    head = pl.ds(0, 8)
    pieces = [
        (up.at[pl.ds(0, HEAD)], up_h), (qmr.at[pl.ds(0, HEAD)], qmr_h), (qse.at[head], qse_h), (kmr.at[head], kmr_h),
        (kse.at[head], kse_h), (vse.at[head], vse_h), (kse.at[tail], kse_t), (vse.at[tail], vse_t),
    ]
    copies = [pltpu.make_async_copy(src, dst, sems.at[k]) for k, (src, dst) in enumerate(pieces)]
    for copy in copies:
        copy.start()
    for copy in copies:
        copy.wait()

    def step(b, carry):
        c = block(b)
        bwd[:HEAD, c] = (up_h[:, c].astype(F32) * qmr_h[:, c].astype(F32)).astype(BF)
        bwd[HEAD : HEAD + 8, c] = qse_h[:, c]
        bwd[HEAD + 8 : HEAD + 16, c] = kmr_h[:, c]
        bwd[HEAD + 16 :, c] = (kse_h[:, c].astype(F32) * vse_h[:, c].astype(F32)).astype(BF)
        fwd[:, c] = (kse_t[:, c].astype(F32) * vse_t[:, c].astype(F32)).astype(BF)
        return carry

    lax.fori_loop(0, fwd.shape[1] // CB, step, 0)


def local_kernel(
    up, qmr, kse, vse, qse, fse, fmr_in, fxh_in, fxl_in, gloc, hspec, conv_o, mixed_o, acc_o, p_o, g_o,
    prod, fmr, fxh, fxl, sems
):
    pieces = ((fmr_in, fmr), (fxh_in, fxh), (fxl_in, fxl))
    copies = [pltpu.make_async_copy(src, dst, sems.at[k]) for k, (src, dst) in enumerate(pieces)]
    for copy in copies:
        copy.start()
    acc_o[...] = jnp.zeros_like(acc_o)
    prod[:, :8] = jnp.zeros((CB // 128, 8, 128), F32)
    steps = up.shape[1] // CB

    def short(b, carry):
        c = block(b)
        product = rounded(kse[:, c].astype(F32) * vse[:, c].astype(F32))
        keep(prod, slice(8, None), product)
        p_o[:, c] = product
        taps = fse[:, c]
        for at in range(0, ROWS, CHUNK):
            conv = short_conv(prod, taps, 8 + at, CHUNK)
            mixed = qse[at : at + CHUNK, c].astype(F32) * conv
            conv_o[at : at + CHUNK, c] = conv
            mixed_o[at : at + CHUNK, c] = mixed
            square = folded(mixed * mixed)
            if at == 0:
                acc_o[8:CHUNK] += square[8:]
            else:
                acc_o[at : at + CHUNK] += square
        return carry

    lax.fori_loop(0, steps, short, 0)
    for copy in copies:
        copy.wait()

    def spectra(b, carry):
        c = block(b)
        g = (up[:, c].astype(F32) * qmr[:, c].astype(F32)).astype(BF)
        g_o[:, c] = g.astype(F32)
        gloc[:, c] = forward(fxh[...], fxl[...], g)
        high, low = split(fmr[:, c])
        fh = fxh[:, :128]
        hspec[:, c] = dot(fh, high) + dot(fxl[:, :128], high) + dot(fh, low)
        return carry

    lax.fori_loop(0, steps, spectra, 0)


def norm_kernel(
    fwd, bwd, p, g_in, qse, kmr, fse, gain, skip, gloc, hspec, mixed, acc_in, fhh, th,
    gp_o, gext_o, conv_e, mixed_e, stats, prod, acc_sq, acc_w
):
    acc_sq[...] = acc_in[...]
    acc_w[...] = jnp.zeros_like(acc_w)

    def step(b, carry):
        c = block(b)
        spec = gloc[:, c] + dot(fhh[...], bwd[:HEAD, c])
        gext_o[:, c] = spec
        h = hspec[:, c]
        gr, gi, hr, hi = spec[:HALF], spec[HALF:], h[:HALF], h[HALF:]
        back = jnp.concatenate([(gr * hr + gi * hi).astype(BF), (gi * hr - gr * hi).astype(BF)], 0)
        gp_o[:, c] = dot(th[...], back)
        taps, gains, skips = fse[:, c], gain[:, c], skip[:, c]
        keep(prod, slice(0, 8), fwd[:, c].astype(F32))
        keep(prod, slice(8, 16), p[:8, c])
        keep(prod, slice(16, 24), p[ROWS - 8 :, c])
        keep(prod, slice(24, 32), bwd[HEAD + 16 :, c].astype(F32))
        edges = []
        for k, query in ((0, qse[:8, c]), (1, bwd[HEAD : HEAD + 8, c])):
            conv = short_conv(prod, taps, 8 + 16 * k, 8)
            edge = query.astype(F32) * conv
            conv_e[8 * k : 8 * k + 8, c] = conv
            mixed_e[8 * k : 8 * k + 8, c] = edge
            edges.append(edge)
            at = ROWS * k
            acc_sq[at : at + 8] += folded(edge * edge)

        def rows(at, count, mix, key, g):
            gp = gp_o[at : at + count, c] + skips * g
            gp_o[at : at + count, c] = gp
            acc_w[at : at + count] += folded(gp * key.astype(F32) * gains * mix)

        for at in range(0, ROWS, CHUNK):
            s = slice(at, at + CHUNK)
            mix = mixed[s, c]
            if at == 0:
                mix = jnp.concatenate([edges[0], mix[8:]], 0)
            rows(at, CHUNK, mix, kmr[s, c], g_in[s, c])
        rows(ROWS, 8, edges[1], bwd[HEAD + 8 : HEAD + 16, c], bwd[:8, c].astype(F32))
        return carry

    lax.fori_loop(0, gloc.shape[1] // CB, step, 0)
    sq = sums_in_lanes(acc_sq[...])
    w = sums_in_lanes(acc_w[...])
    mine = jnp.concatenate([sq[:1, :128], sq[:1, 128:], w[:1, :128], w[:1, 128:], jnp.zeros((4, 128), F32)], 0)
    for dev in range(8):
        stats[dev] = mine


def column(total, row):
    pick = (lax.broadcasted_iota(jnp.int32, (8, 128), 0) == row).astype(F32)
    return lax.dot_general(
        total, pick, (((0,), (0,)), ((), ())), precision=lax.Precision.HIGHEST, preferred_element_type=F32
    )


def merged_rows(body, edge, at, count, c=slice(None)):
    rows = body[at : at + count, c]
    return jnp.concatenate([edge[:8, c], rows[8:]], 0) if at == 0 else rows


def scales(stats, scale_s, coef_s):
    total = stats[0]
    for dev in range(1, 8):
        total = total + stats[dev]
    s0 = lax.rsqrt(column(total, 0) / D + EPSILON)
    s1 = lax.rsqrt(column(total, 1) / D + EPSILON)
    scale_s[:128] = s0
    scale_s[128:] = s1
    coef_s[:128] = s0 * s0 * s0 * (column(total, 2) / D)
    coef_s[128:] = s1 * s1 * s1 * (column(total, 3) / D)


def filter_kernel(
    stats, fwd, p, g_in, mixed, mixed_e, gp, kmr, qse, gain, gext, fxh, th, spots,
    payload, halo, prod, small, scale_s, coef_s, pms
):
    steps = gext.shape[1] // CB
    scales(stats, scale_s, coef_s)

    def step(b, carry):
        c = block(b)
        keep(prod, slice(0, 8), fwd[:, c].astype(F32))
        keep(prod, slice(8, None), p[:, c])
        gains = gain[:, c]
        sums = [jnp.zeros((8, CB), F32) for _ in range(9)]
        for at in range(0, ROWS, CHUNK):
            s = slice(at, at + CHUNK)
            mix = merged_rows(mixed, mixed_e, at, CHUNK, c)
            scale = wide(scale_s[s])
            key = kmr[s, c].astype(F32)
            grad = gp[s, c]
            gn = grad * key
            ms = mix * scale
            normed = ms * gains
            pm = (key * normed).astype(BF)
            pms[s] = pm
            if at >= ROWS - HALO:
                halo[at - (ROWS - HALO) : at - (ROWS - HALO) + CHUNK, c] = pm
            gm = gains * scale * gn - mix * wide(coef_s[s])
            gc = rounded(gm * qse[s, c].astype(F32))
            for tap in range(7):
                sums[tap] = sums[tap] + eights(gc * shifted(prod, 8 + at - tap, CHUNK))
            sums[7] = sums[7] + eights(g_in[s, c] * pm.astype(F32))
            sums[8] = sums[8] + eights(gn * ms)
        parts = [jnp.sum(x, axis=0, keepdims=True) for x in sums]
        small[b] = jnp.concatenate(parts + [jnp.zeros((7, CB), F32)], 0)

        x = dot(fxh[...], pms[...])
        ge = gext[:, c]
        xr, xi, gr, gi = x[:HALF], x[HALF:], ge[:HALF], ge[HALF:]
        back = jnp.concatenate([(gr * xr + gi * xi).astype(BF), (gi * xr - gr * xi).astype(BF)], 0)
        corr = dot(th[:128], back).T.astype(BF)
        for zz in range(4):
            for yc in range(4):
                at = pl.multiple_of((4 * b + zz) * 16, 16)
                payload[yc, pl.ds(at, 16), :] = corr[zz * 64 + yc * 16 : zz * 64 + yc * 16 + 16]
        return carry

    lax.fori_loop(0, steps, step, 0)

    lane = lax.broadcasted_iota(jnp.int32, (16, 128), 1)
    row = lax.broadcasted_iota(jnp.int32, (16, 128), 0)
    spread = (lane % 16 == row).astype(BF)
    chan = lax.broadcasted_iota(jnp.int32, (CB, 128), 0)
    own = chan % 8 == lax.broadcasted_iota(jnp.int32, (CB, 128), 1) // 16
    packed = None
    for b in range(steps):
        tiled = lax.dot_general(
            small[b].astype(BF), spread, (((0,), (0,)), ((), ())), preferred_element_type=F32
        )
        masked = jnp.where(own, tiled, 0.0).astype(BF)
        part = dot(spots[:, b * CB : b * CB + CB], masked)
        packed = part if packed is None else packed + part
    packed = packed.astype(BF)
    for yc in range(4):
        payload[yc, 256:] = packed[yc * 32 : yc * 32 + 32]


def rest_kernel(
    stats, mixed, conv, mixed_e, conv_e, gp, bwd, kmr, kse, vse, qse, gain, fse,
    gqse, gkse, gvse, gkmr, pm_o, scale_s, coef_s, gcs
):
    @pl.when(pl.program_id(0) == 0)
    def _():
        scales(stats, scale_s, coef_s)

    gains, taps = gain[...], fse[...]
    for at in range(0, ROWS, CHUNK):
        s = slice(at, at + CHUNK)
        mix = merged_rows(mixed, mixed_e, at, CHUNK)
        con = merged_rows(conv, conv_e, at, CHUNK)
        scale, key, grad = wide(scale_s[s]), kmr[s].astype(F32), gp[s]
        normed = mix * scale * gains
        pm_o[s] = (key * normed).astype(BF)
        gkmr[s] = (grad * normed).astype(BF)
        gm = gains * scale * (grad * key) - mix * wide(coef_s[s])
        gqse[s] = (gm * con).astype(BF)
        keep(gcs, s, rounded(gm * qse[s].astype(F32)))
    nxt = slice(ROWS, ROWS + 8)
    gn = gp[nxt] * bwd[HEAD + 8 : HEAD + 16].astype(F32)
    gm = gains * wide(scale_s[nxt]) * gn - mixed_e[8:] * wide(coef_s[nxt])
    keep(gcs, nxt, rounded(gm * bwd[HEAD : HEAD + 8].astype(F32)))
    for at in range(0, ROWS, CHUNK):
        s = slice(at, at + CHUNK)
        gps = short_adjoint(gcs, taps, at, CHUNK)
        gkse[s] = (gps * vse[s].astype(F32)).astype(BF)
        gvse[s] = (gps * kse[s].astype(F32)).astype(BF)


def query_kernel(
    halo, pm_in, hspec_in, up_in, skip, fxh, fhalo, th, gqmr, pm, hspec, up, out, sems
):
    steps = pm.shape[1] // CB

    def copies(b):
        c = block(b)
        pairs = ((pm_in, pm), (hspec_in, hspec), (up_in, up))
        return [pltpu.make_async_copy(src.at[:, c], dst.at[:, c], sems.at[k, b]) for k, (src, dst) in enumerate(pairs)]

    def out_copy(b):
        c = block(b)
        return pltpu.make_async_copy(out.at[:, c], gqmr.at[:, c], sems.at[3, b])

    for b in range(steps):
        for copy in copies(b):
            copy.start()

    def step(b, carry):
        for copy in copies(b):
            copy.wait()
        c = block(b)
        x, h = dot(fxh[...], pm[:, c]) + dot(fhalo[...], halo[:, c]), hspec[:, c]
        xr, xi, hr, hi = x[:HALF], x[HALF:], h[:HALF], h[HALF:]
        spec = jnp.concatenate([(xr * hr - xi * hi).astype(BF), (xi * hr + xr * hi).astype(BF)], 0)
        ym = dot(th[...], spec)
        for at in range(0, ROWS, CHUNK):
            s = slice(at, at + CHUNK)
            out[s, c] = (up[s, c].astype(F32) * (ym[s] + skip[:, c] * pm[s, c].astype(F32))).astype(BF)
        out_copy(b).start()
        return carry

    lax.fori_loop(0, steps, step, 0)
    for b in range(steps):
        out_copy(b).wait()


def merge_kernel(got, out):
    total = got[0].astype(F32)
    for k in range(1, 4):
        total = total + got[k].astype(F32)
    for z in range(16):
        for k in range(9):
            at = z * 16 + 2 * k if k < 8 else 256 + 2 * z
            out[z, :, 128 * k : 128 * k + 128] = total[at : at + 2].astype(BF)


def final_kernel(got, se_o, mr_o, skip_o, gain_o, *, factor):
    packed = got[0].astype(F32)
    for k in range(1, 16):
        packed = packed + got[k].astype(F32)
    total = jnp.concatenate([packed[:, 128 * k : 128 * k + 128] for k in range(9)], 0)
    total = total * factor
    mr_o[...] = total[:16]
    chan = lax.broadcasted_iota(jnp.int32, (16, 128), 0)
    lane = lax.broadcasted_iota(jnp.int32, (16, 128), 1)
    mine = jnp.where(chan < 8, total[16:17], total[17:18])
    mine = jnp.where(lane // 16 == chan % 8, mine, 0.0)
    pick = (lane % 16 == chan).astype(F32)
    small = lax.dot_general(
        pick, mine, (((1,), (1,)), ((), ())), precision=lax.Precision.HIGHEST, preferred_element_type=F32
    )
    se_o[...] = small[:7]
    skip_o[...] = small[7:8]
    gain_o[...] = small[8:9]


def local(
    query_se, key_se, value_se, query_mr, key_mr, upstream, filter_se, filter_mr, skip_mr, norm_gain
):
    chans = query_se.shape[1]
    steps = chans // CB
    size = lax.axis_size("ctx")
    skip2, gain2 = skip_mr.reshape(1, chans), norm_gain.reshape(1, chans)
    fxh, fxl = halves(basis(0, ROWS))
    fhead, _ = halves(basis(ROWS, ROWS + HEAD))
    fhalo, _ = halves(basis(-HALO, 0))
    back, _ = halves(basis(0, EXT).T * (2.0 / LEN))

    def shape(rows, dtype):
        return jax.ShapeDtypeStruct((rows, chans), dtype)

    def vmem(rows, width, dtype):
        return pltpu.VMEM((rows, width), dtype)

    def shifts(rows):
        return pltpu.VMEM((CB // 128, rows, 128), F32)

    def kept(x):
        return pltpu.with_memory_space_constraint(x, pltpu.HBM)

    params = pltpu.CompilerParams(vmem_limit_bytes=16 * 1024 * 1024)
    hbm = pl.BlockSpec(memory_space=pltpu.HBM)
    here = pl.BlockSpec(memory_space=pltpu.VMEM)
    fwd, bwd = pl.pallas_call(
        send_kernel,
        in_specs=[hbm] * 6,
        out_shape=[shape(8, BF), shape(BWD, BF)],
        scratch_shapes=[vmem(HEAD, chans, BF)] * 2 + [vmem(8, chans, BF)] * 6 + [pltpu.SemaphoreType.DMA((8,))],
        compiler_params=params,
        name="send",
    )(*(kept(x) for x in (key_se, value_se, query_se, key_mr, upstream, query_mr)))

    down = [(k, k + 1) for k in range(size - 1)]
    upward = [(k + 1, k) for k in range(size - 1)]
    bwd = lax.ppermute(bwd, "ctx", upward)
    fwd = lax.ppermute(fwd, "ctx", down)

    gloc, hspec, conv, mixed, acc, p, g = pl.pallas_call(
        local_kernel,
        in_specs=[here] * 6 + [hbm] * 3,
        out_shape=[shape(LEN, F32), shape(LEN, F32), shape(ROWS, F32), shape(ROWS, F32),
                   jax.ShapeDtypeStruct((256, 128), F32), shape(ROWS, F32), shape(ROWS, F32)],
        scratch_shapes=[shifts(ROWS + 8), vmem(filter_mr.shape[0], chans, F32), vmem(LEN, ROWS, BF),
                        vmem(LEN, ROWS, BF), pltpu.SemaphoreType.DMA((3,))],
        compiler_params=params,
        name="local",
    )(upstream, query_mr, key_se, value_se, query_se, filter_se, kept(filter_mr), kept(fxh), kept(fxl))

    gp, gext, conv_e, mixed_e, stats = pl.pallas_call(
        norm_kernel,
        out_shape=[shape(EXT, F32), shape(LEN, F32), shape(16, F32), shape(16, F32),
                   jax.ShapeDtypeStruct((8, 8, 128), F32)],
        scratch_shapes=[shifts(32), vmem(256, 128, F32), vmem(256, 128, F32)],
        compiler_params=params,
        name="norm",
    )(fwd, bwd, p, g, query_se, key_mr, filter_se, gain2, skip2, gloc, hspec,
      mixed, acc, fhead, back)

    stats = lax.all_to_all(stats, "tp", 0, 0, tiled=True)

    payload, halo = pl.pallas_call(
        filter_kernel,
        out_shape=[jax.ShapeDtypeStruct((4, 288, 128), BF), shape(HALO, BF)],
        scratch_shapes=[shifts(ROWS + 8), pltpu.VMEM((steps, 16, CB), F32), vmem(256, 128, F32), vmem(256, 128, F32),
                        vmem(ROWS, CB, BF)],
        compiler_params=params,
        name="filters",
    )(stats, fwd, p, g, mixed, mixed_e, gp, key_mr, query_se, gain2, gext, fxh, back, owner_rows(chans).astype(BF))
    halo = lax.ppermute(halo, "ctx", down)

    def cols(rows):
        return pl.BlockSpec((rows, CB), lambda i: (0, i))

    def whole(*dims):
        return pl.BlockSpec(dims, lambda i: (0,) * len(dims))

    late = (mixed, conv, mixed_e, conv_e, gp, bwd, key_mr, key_se, value_se, query_se, gain2, filter_se)
    gqse, gkse, gvse, gkmr, pm = pl.pallas_call(
        rest_kernel,
        grid=(steps,),
        in_specs=[whole(8, 8, 128)] + [cols(x.shape[0]) for x in late],
        out_specs=[cols(ROWS)] * 5,
        out_shape=[shape(ROWS, BF)] * 4 + [pltpu.HBM((ROWS, chans), BF)],
        scratch_shapes=[vmem(256, 128, F32), vmem(256, 128, F32), shifts(EXT)],
        compiler_params=params,
        name="rest",
    )(kept(stats), *(kept(x) for x in late))
    gqmr = pl.pallas_call(
        query_kernel,
        in_specs=[here] + [hbm] * 3 + [here] * 4,
        out_specs=hbm,
        out_shape=shape(ROWS, BF),
        scratch_shapes=[vmem(ROWS, chans, BF), vmem(LEN, chans, F32), vmem(ROWS, chans, BF), vmem(ROWS, chans, BF),
                        pltpu.SemaphoreType.DMA((4, steps))],
        compiler_params=params,
        name="query",
    )(halo, kept(pm), kept(hspec), kept(upstream), skip2, fxh, fhalo, back)

    near = [[4 * a + b for b in range(4)] for a in range(size // 4)]
    far = [[4 * a + b for a in range(size // 4)] for b in range(4)]
    got = lax.all_to_all(payload, "ctx", 0, 0, axis_index_groups=near, tiled=True)
    merged = pl.pallas_call(
        merge_kernel, out_shape=jax.ShapeDtypeStruct((16, 2, 1152), BF), compiler_params=params, name="merge"
    )(got)
    got = lax.all_to_all(merged, "ctx", 0, 0, axis_index_groups=far, tiled=True)
    factor = 1.0 / math.sqrt(ROWS * size)
    se, mr, sk, ga = pl.pallas_call(
        lambda *refs: final_kernel(*refs, factor=factor),
        out_shape=[jax.ShapeDtypeStruct((7, 16), F32), jax.ShapeDtypeStruct((16, 128), F32),
                   jax.ShapeDtypeStruct((1, 16), F32), jax.ShapeDtypeStruct((1, 16), F32)],
        compiler_params=params,
        name="final",
    )(got)
    return (gqse, gkse, gvse, gqmr, gkmr, se, mr.T, sk.reshape(16), ga.reshape(16))


def solution(mesh):
    both, part = P("ctx", "tp"), P(None, "tp")
    in_specs = (both,) * 6 + (part, part, P("tp"), P("tp"))
    split_all = ("tp", "ctx")
    out_specs = (both,) * 5 + (P(None, split_all), P(None, split_all), P(split_all), P(split_all))
    return jax.shard_map(local, mesh=mesh, in_specs=in_specs, out_specs=out_specs, check_vma=False)
```
